32 devices in a mesh: dp: 4 (over y, z), tp: 8 (over x, core).
Axes of the slice: x: 4, y: 2, z: 2, core: 2. Of those that a mesh axis runs over, the one named last changes fastest.
The devices are a block of a 4x4x8 slice.
Arguments:
- hidden_in: bfloat16 [4096, 2048], P(('dp', 'tp')), parts along dimension 0
- k_cache: bfloat16 [4096, 256, 256], P(('dp', 'tp')), parts along dimension 0
- v_cache: bfloat16 [4096, 256, 256], P(('dp', 'tp')), parts along dimension 0
- cache_len: int32 [4096], P(('dp', 'tp')), parts along dimension 0
- norm_attn: bfloat16 [2048], replicated
- norm_mlp: bfloat16 [2048], replicated
- w_q: bfloat16 [2048, 2048], replicated
- w_k: bfloat16 [2048, 256], replicated
- w_v: bfloat16 [2048, 256], replicated
- w_o: bfloat16 [2048, 2048], replicated
- w_gate: bfloat16 [2048, 16384], P(None, 'tp')
- w_up: bfloat16 [2048, 16384], P(None, 'tp')
- w_down: bfloat16 [16384, 2048], P('tp')
Outputs:
- output 1: bfloat16 [4096, 2048], P(('dp', 'tp')), parts along dimension 0
- output 2: bfloat16 [4096, 256], P(('dp', 'tp')), parts along dimension 0
- output 3: bfloat16 [4096, 256], P(('dp', 'tp')), parts along dimension 0
There are 4 independent parts. The reference program is written for one: setup_inputs(seed, part) draws one part's arguments, and reference() takes and returns one part's arrays. A program takes and returns all parts, laid end to end along the dimension named above; an argument that names none is the same for every part.
All inputs are finite; a program needn't handle non-finite values.
Results may differ from the reference program's by a relative error of at most 0.00561948.
Values are sent between devices in bfloat16 or wider.
A program may use at most 768 MiB of HBM per device.

```python
import jax
import jax.numpy as jnp
from jax import lax

D_MODEL = 2048
NUM_HEADS = 8
HEAD_DIM = 256
FF_DIM = 16384
BATCH_ROWS = 1024
CACHE_SIZE = 256


def scaled_normal(key_w, shape_w, fan_in):
    return (jax.random.normal(key_w, shape_w, jnp.float32) * fan_in ** -0.5).astype(jnp.bfloat16)


def setup_inputs(seed: int = 0, part: int = 0) -> dict:
    base_key = jax.random.key(seed)
    shared_keys = jax.random.split(base_key, 9)
    own_keys = jax.random.split(jax.random.fold_in(base_key, part), 5)
    q_width = NUM_HEADS * HEAD_DIM
    hidden_in = jax.random.normal(own_keys[0], (BATCH_ROWS, D_MODEL), jnp.float32)
    k_cache = 2.0 * jax.random.normal(own_keys[1], (BATCH_ROWS, CACHE_SIZE, HEAD_DIM), jnp.float32)
    v_mean = 0.7 * jax.random.normal(own_keys[2], (BATCH_ROWS, 1, HEAD_DIM), jnp.float32)
    v_cache = v_mean + jax.random.normal(own_keys[3], (BATCH_ROWS, CACHE_SIZE, HEAD_DIM), jnp.float32)
    cache_len = jax.random.randint(own_keys[4], (BATCH_ROWS,), 0, CACHE_SIZE, jnp.int32)
    cache_len = cache_len.at[0].set(CACHE_SIZE - 1)
    return {
        'hidden_in': hidden_in.astype(jnp.bfloat16),
        'k_cache': k_cache.astype(jnp.bfloat16),
        'v_cache': v_cache.astype(jnp.bfloat16),
        'cache_len': cache_len,
        'norm_attn': (0.3 * jax.random.normal(shared_keys[0], (D_MODEL,), jnp.float32)).astype(jnp.bfloat16),
        'norm_mlp': (0.3 * jax.random.normal(shared_keys[1], (D_MODEL,), jnp.float32)).astype(jnp.bfloat16),
        'w_q': scaled_normal(shared_keys[2], (D_MODEL, q_width), D_MODEL),
        'w_k': scaled_normal(shared_keys[3], (D_MODEL, HEAD_DIM), D_MODEL),
        'w_v': scaled_normal(shared_keys[4], (D_MODEL, HEAD_DIM), D_MODEL),
        'w_o': scaled_normal(shared_keys[5], (q_width, D_MODEL), q_width),
        'w_gate': scaled_normal(shared_keys[6], (D_MODEL, FF_DIM), D_MODEL),
        'w_up': scaled_normal(shared_keys[7], (D_MODEL, FF_DIM), D_MODEL),
        'w_down': scaled_normal(shared_keys[8], (FF_DIM, D_MODEL), FF_DIM),
    }


def rms_scale(values, gain_vec):
    wide_vals = values.astype(jnp.float32)
    inv_rms = lax.rsqrt(jnp.mean(wide_vals * wide_vals, axis=-1, keepdims=True) + 1e-6)
    return (wide_vals * inv_rms * (1.0 + gain_vec.astype(jnp.float32))).astype(jnp.bfloat16)


def rope_tables(positions, head_dim):
    half_dim = head_dim // 2
    inv_freq = 10000.0 ** (-2.0 * jnp.arange(half_dim, dtype=jnp.float32) / head_dim)
    angles = positions.astype(jnp.float32)[:, None] * inv_freq[None, :]
    return jnp.cos(angles), jnp.sin(angles)


def rotary(values, cos_t, sin_t):
    half_dim = values.shape[-1] // 2
    first_half = values[..., :half_dim]
    second_half = values[..., half_dim:]
    return jnp.concatenate([first_half * cos_t - second_half * sin_t, second_half * cos_t + first_half * sin_t], axis=-1)


def attend_row(row_args):
    q_row, k_row, v_row, k_hist, v_hist, position = row_args
    q_wide = q_row.astype(jnp.float32)
    hist_score = jnp.einsum('hd,td->ht', q_wide, k_hist.astype(jnp.float32))
    new_score = jnp.einsum('hd,d->h', q_wide, k_row.astype(jnp.float32))
    valid_mask = jnp.arange(k_hist.shape[0]) < position
    hist_score = jnp.where(valid_mask[None, :], hist_score, -jnp.inf)
    peak_score = jnp.maximum(jnp.max(hist_score, axis=-1), new_score)
    hist_weight = jnp.exp(hist_score - peak_score[:, None])
    new_weight = jnp.exp(new_score - peak_score)
    weight_sum = jnp.sum(hist_weight, axis=-1) + new_weight
    hist_prob = (hist_weight / weight_sum[:, None]).astype(jnp.bfloat16)
    new_prob = (new_weight / weight_sum).astype(jnp.bfloat16)
    attn_out = jnp.einsum('ht,td->hd', hist_prob.astype(jnp.float32), v_hist.astype(jnp.float32))
    attn_out = attn_out + new_prob.astype(jnp.float32)[:, None] * v_row.astype(jnp.float32)[None, :]
    return attn_out.astype(jnp.bfloat16)


def reference(hidden_in, k_cache, v_cache, cache_len, norm_attn, norm_mlp, w_q, w_k, w_v, w_o, w_gate, w_up, w_down):
    num_rows = hidden_in.shape[0]
    normed = rms_scale(hidden_in, norm_attn)
    q_lin = jnp.dot(normed, w_q, preferred_element_type=jnp.float32).reshape(num_rows, NUM_HEADS, HEAD_DIM)
    k_lin = jnp.dot(normed, w_k, preferred_element_type=jnp.float32)
    v_new = jnp.dot(normed, w_v, preferred_element_type=jnp.float32).astype(jnp.bfloat16)
    cos_t, sin_t = rope_tables(cache_len, HEAD_DIM)
    q_rot = (rotary(q_lin, cos_t[:, None, :], sin_t[:, None, :]) * HEAD_DIM ** -0.5).astype(jnp.bfloat16)
    k_new = rotary(k_lin, cos_t, sin_t).astype(jnp.bfloat16)
    attn_out = lax.map(attend_row, (q_rot, k_new, v_new, k_cache, v_cache, cache_len))
    mixed = jnp.dot(attn_out.reshape(num_rows, NUM_HEADS * HEAD_DIM), w_o, preferred_element_type=jnp.float32)
    x_mid = hidden_in.astype(jnp.float32) + mixed
    xn_mid = rms_scale(x_mid, norm_mlp)
    gate_act = jnp.dot(xn_mid, w_gate, preferred_element_type=jnp.float32)
    up_act = jnp.dot(xn_mid, w_up, preferred_element_type=jnp.float32)
    hidden_act = (jax.nn.gelu(gate_act, approximate=True) * up_act).astype(jnp.bfloat16)
    down_sum = jnp.dot(hidden_act, w_down, preferred_element_type=jnp.float32)
    hidden_out = (x_mid + down_sum).astype(jnp.bfloat16)
    return hidden_out, k_new, v_new
```

```python
import functools

import jax
import jax.numpy as jnp
from jax import lax
from jax.experimental import pallas as pl
from jax.experimental.pallas import tpu as pltpu
from jax.sharding import PartitionSpec as P

MESH = pl.DeviceIdType.MESH


def rms_scale(values, gain_vec):
    wide_vals = values.astype(jnp.float32)
    inv_rms = lax.rsqrt(jnp.mean(wide_vals * wide_vals, axis=-1, keepdims=True) + 1e-6)
    return (wide_vals * inv_rms * (1.0 + gain_vec.astype(jnp.float32))).astype(jnp.bfloat16)


def rope_tables(positions, head_dim):
    half_dim = head_dim // 2
    inv_freq = 10000.0 ** (-2.0 * jnp.arange(half_dim, dtype=jnp.float32) / head_dim)
    angles = positions.astype(jnp.float32)[:, None] * inv_freq[None, :]
    return jnp.cos(angles), jnp.sin(angles)


def rotary(values, cos_t, sin_t):
    half_dim = values.shape[-1] // 2
    first_half = values[..., :half_dim]
    second_half = values[..., half_dim:]
    return jnp.concatenate([first_half * cos_t - second_half * sin_t, second_half * cos_t + first_half * sin_t], axis=-1)


def attend(q_rot, k_new, v_new, k_cache, v_cache, cache_len):
    hist_score = jnp.einsum('bhd,btd->bht', q_rot, k_cache, preferred_element_type=jnp.float32)
    new_score = jnp.einsum('bhd,bd->bh', q_rot, k_new, preferred_element_type=jnp.float32)
    valid_mask = lax.broadcasted_iota(jnp.int32, (1, 1, k_cache.shape[1]), 2) < cache_len[:, None, None]
    hist_score = jnp.where(valid_mask, hist_score, -jnp.inf)
    peak_score = jnp.maximum(jnp.max(hist_score, axis=-1), new_score)
    hist_weight = jnp.exp(hist_score - peak_score[..., None])
    new_weight = jnp.exp(new_score - peak_score)
    weight_sum = jnp.sum(hist_weight, axis=-1) + new_weight
    hist_prob = (hist_weight / weight_sum[..., None]).astype(jnp.bfloat16)
    new_prob = (new_weight / weight_sum).astype(jnp.bfloat16)
    attn_out = jnp.einsum('bht,btd->bhd', hist_prob, v_cache, preferred_element_type=jnp.float32)
    attn_out = attn_out + new_prob.astype(jnp.float32)[..., None] * v_new.astype(jnp.float32)[:, None, :]
    return attn_out.astype(jnp.bfloat16)


def attention_block(hidden_in, k_cache, v_cache, cache_len, norm_attn, w_q, w_k, w_v, w_o):
    num_rows = hidden_in.shape[0]
    head_dim = w_k.shape[1]
    num_heads = w_q.shape[1] // head_dim
    normed = rms_scale(hidden_in, norm_attn)
    q_lin = jnp.dot(normed, w_q, preferred_element_type=jnp.float32).reshape(num_rows, num_heads, head_dim)
    k_lin = jnp.dot(normed, w_k, preferred_element_type=jnp.float32)
    v_new = jnp.dot(normed, w_v, preferred_element_type=jnp.float32).astype(jnp.bfloat16)
    cos_t, sin_t = rope_tables(cache_len, head_dim)
    q_rot = (rotary(q_lin, cos_t[:, None, :], sin_t[:, None, :]) * head_dim ** -0.5).astype(jnp.bfloat16)
    k_new = rotary(k_lin, cos_t, sin_t).astype(jnp.bfloat16)
    attn_out = attend(q_rot, k_new, v_new, k_cache, v_cache, cache_len)
    mixed = jnp.dot(attn_out.reshape(num_rows, num_heads * head_dim), w_o, preferred_element_type=jnp.float32)
    return hidden_in.astype(jnp.float32) + mixed, k_new, v_new


def mlp_kernel(half, tile, depth_tile, xn_ref, x_ref, wg_hbm, wu_hbm, wd_hbm, out_ref,
               wg, wu, wd, xb, hid, own, snd, prt, ring,
               w_sem, ag_send, ag_recv, d_send, d_recv, r_send, r_recv):
    chips = lax.axis_size('tp') // 2
    me = lax.axis_index('tp')
    core = lax.rem(me, 2)
    chip = me // 2
    partner = me + 1 - 2 * core
    ahead = 2 * lax.rem(chip + 1, chips) + core
    behind = 2 * lax.rem(chip + chips - 1, chips) + core
    rows = 2 * half
    n_up = wg.shape[0]
    n_down = wd.shape[0]

    def to(src, dst, send, recv, dev):
        return pltpu.make_async_remote_copy(src_ref=src, dst_ref=dst, send_sem=send, recv_sem=recv,
                                            device_id={'tp': dev}, device_id_type=MESH)

    barrier = pltpu.get_barrier_semaphore()
    for dev in (partner, ahead, behind):
        pl.semaphore_signal(barrier, inc=1, device_id={'tp': dev}, device_id_type=MESH)

    def up_load(i, n):
        src, dst = ((wg_hbm, wg), (wu_hbm, wu))[i]
        return pltpu.make_async_copy(src.at[:, pl.ds(n * tile, tile)], dst.at[n], w_sem.at[i, n])

    def down_load(n):
        return pltpu.make_async_copy(wd_hbm.at[:, pl.ds(n * depth_tile, depth_tile)], wd.at[n], w_sem.at[2, n])

    for n in range(n_up):
        up_load(0, n).start()
        up_load(1, n).start()
    for n in range(n_down):
        down_load(n).start()

    lo, hi = pl.ds(0, half), pl.ds(half, half)
    mine, theirs = pl.ds(0, rows), pl.ds(rows, rows)
    pl.semaphore_wait(barrier, 3)

    gather = [
        to(xn_ref, xb.at[0, theirs], ag_send.at[0], ag_recv.at[0], partner),
        to(xn_ref.at[lo], xb.at[1, hi], ag_send.at[1], ag_recv.at[1], ahead),
        to(xn_ref.at[hi], xb.at[1, lo], ag_send.at[2], ag_recv.at[2], behind),
        to(xn_ref.at[hi], xb.at[2, hi], ag_send.at[3], ag_recv.at[3], ahead),
        to(xn_ref.at[lo], xb.at[2, lo], ag_send.at[4], ag_recv.at[4], behind),
        to(xb.at[1, hi], xb.at[3, lo], ag_send.at[5], ag_recv.at[5], ahead),
        to(xb.at[1, lo], xb.at[3, hi], ag_send.at[6], ag_recv.at[6], behind),
        to(xb.at[1, mine], xb.at[1, theirs], ag_send.at[7], ag_recv.at[7], partner),
        to(xb.at[2, mine], xb.at[2, theirs], ag_send.at[8], ag_recv.at[8], partner),
        to(xb.at[3, mine], xb.at[3, theirs], ag_send.at[9], ag_recv.at[9], partner),
    ]
    for copy in gather[:5]:
        copy.start()
    xb[0, 0:rows, :] = xn_ref[...]

    def up(b):
        def body(n, carry):
            if b == 0:
                up_load(0, n).wait()
                up_load(1, n).wait()
            gate = jnp.dot(xb[b], wg[n], preferred_element_type=jnp.float32)
            lin = jnp.dot(xb[b], wu[n], preferred_element_type=jnp.float32)
            act = jax.nn.gelu(gate, approximate=True) * lin
            hid[:, pl.ds(pl.multiple_of(n * tile, tile), tile)] = act.astype(jnp.bfloat16)
            return carry
        lax.fori_loop(0, n_up, body, 0)

    def exchange(b, n):
        return to(snd.at[b, n], prt.at[b, n], d_send.at[b, n], d_recv.at[b, n], partner)

    def hops(step, b, n):
        return (to(own.at[b, n, lo], ring.at[step, n, lo], r_send.at[step, 0, n], r_recv.at[step, 0, n], ahead),
                to(own.at[b, n, hi], ring.at[step, n, hi], r_send.at[step, 1, n], r_recv.at[step, 1, n], behind))

    def merge(b, n, step):
        exchange(b, n).wait_recv()
        own[b, n] = own[b, n] + prt[b, n]
        if step is not None:
            for copy in hops(step, b, n):
                copy.start()

    def down(b, step):
        def body(n, carry):
            if b == 0:
                down_load(n).wait()
            part = jnp.dot(hid[...], wd[n], preferred_element_type=jnp.float32)
            own[b, n] = part[0:rows]
            snd[b, n] = part[rows:2 * rows]
            exchange(b, n).start()
            @pl.when(n > 0)
            def _():
                merge(b, n - 1, step)
            return carry
        lax.fori_loop(0, n_down, body, 0)
        merge(b, n_down - 1, step)

    gather[0].wait_recv()
    up(0)
    down(0, None)
    gather[1].wait_recv()
    gather[2].wait_recv()
    gather[7].start()
    gather[5].start()
    gather[6].start()
    gather[7].wait_recv()
    up(1)
    gather[3].wait_recv()
    gather[4].wait_recv()
    gather[8].start()
    down(1, 0)
    gather[8].wait_recv()
    up(2)
    gather[5].wait_recv()
    gather[6].wait_recv()
    gather[9].start()
    down(2, None)
    gather[9].wait_recv()
    up(3)
    down(3, 1)

    def relay(n, carry):
        for copy in hops(1, 3, n):
            copy.wait_recv()
        own[2, n] = own[2, n] + ring[1, n]
        for copy in hops(2, 2, n):
            copy.start()
        for copy in hops(0, 1, n):
            copy.wait_recv()
        own[0, n, lo] = own[0, n, lo] + ring[0, n, hi]
        own[0, n, hi] = own[0, n, hi] + ring[0, n, lo]
        return carry
    lax.fori_loop(0, n_down, relay, 0)

    def finish(n, carry):
        for copy in hops(2, 2, n):
            copy.wait_recv()
        cols = pl.ds(pl.multiple_of(n * depth_tile, depth_tile), depth_tile)
        out_ref[:, cols] = (x_ref[:, cols] + (own[0, n] + ring[2, n])).astype(jnp.bfloat16)
        return carry
    lax.fori_loop(0, n_down, finish, 0)

    for copy in gather:
        copy.wait_send()
    def drain(n, carry):
        for b in range(4):
            exchange(b, n).wait_send()
        for step, b in ((0, 1), (1, 3), (2, 2)):
            for copy in hops(step, b, n):
                copy.wait_send()
        return carry
    lax.fori_loop(0, n_down, drain, 0)


def mlp(xn, x_mid, w_gate, w_up, w_down):
    rows, width = xn.shape
    units = w_gate.shape[1]
    tile = 512
    depth_tile = 512
    n_up, n_down = units // tile, width // depth_tile
    sems = pltpu.SemaphoreType.DMA
    vmem = pl.BlockSpec(memory_space=pltpu.VMEM)
    hbm = pl.BlockSpec(memory_space=pl.ANY)
    return pl.pallas_call(
        functools.partial(mlp_kernel, rows // 2, tile, depth_tile),
        out_shape=jax.ShapeDtypeStruct((rows, width), jnp.bfloat16),
        in_specs=[vmem, vmem, hbm, hbm, hbm],
        out_specs=vmem,
        scratch_shapes=[
            pltpu.VMEM((n_up, width, tile), jnp.bfloat16),
            pltpu.VMEM((n_up, width, tile), jnp.bfloat16),
            pltpu.VMEM((n_down, units, depth_tile), jnp.bfloat16),
            pltpu.VMEM((4, 2 * rows, width), jnp.bfloat16),
            pltpu.VMEM((2 * rows, units), jnp.bfloat16),
            pltpu.VMEM((4, n_down, rows, depth_tile), jnp.float32),
            pltpu.VMEM((4, n_down, rows, depth_tile), jnp.float32),
            pltpu.VMEM((4, n_down, rows, depth_tile), jnp.float32),
            pltpu.VMEM((3, n_down, rows, depth_tile), jnp.float32),
            sems((3, max(n_up, n_down))),
            sems((10,)), sems((10,)),
            sems((4, n_down)), sems((4, n_down)),
            sems((3, 2, n_down)), sems((3, 2, n_down)),
        ],
        compiler_params=pltpu.CompilerParams(collective_id=0, has_side_effects=True, vmem_limit_bytes=60 * 1024 * 1024),
        cost_estimate=pl.CostEstimate(flops=2 * 8 * rows * width * units * 3, bytes_accessed=6 * width * units, transcendentals=0),
        name='mlp',
    )(xn, x_mid, w_gate, w_up, w_down)


def solution(mesh):
    row_spec = P(('dp', 'tp'), None)
    cache_spec = P(('dp', 'tp'), None, None)
    full_vec = P(None)
    full_mat = P(None, None)

    def per_device(hidden_in, k_cache, v_cache, cache_len, norm_attn, norm_mlp, w_q, w_k, w_v, w_o, w_gate, w_up, w_down):
        x_mid, k_new, v_new = attention_block(hidden_in, k_cache, v_cache, cache_len, norm_attn, w_q, w_k, w_v, w_o)
        xn_mid = rms_scale(x_mid, norm_mlp)
        return mlp(xn_mid, x_mid, w_gate, w_up, w_down), k_new, v_new

    return jax.shard_map(
        per_device,
        mesh=mesh,
        in_specs=(row_spec, cache_spec, cache_spec, P(('dp', 'tp')), full_vec, full_vec,
                  full_mat, full_mat, full_mat, full_mat, P(None, 'tp'), P(None, 'tp'), P('tp', None)),
        out_specs=(row_spec, row_spec, row_spec),
        check_vma=False,
    )
```

```python
import functools

import jax
import jax.numpy as jnp
from jax import lax
from jax.experimental import pallas as pl
from jax.experimental.pallas import tpu as pltpu
from jax.sharding import PartitionSpec as P

MESH = pl.DeviceIdType.MESH


def attn_kernel(group, x_ref, len_ref, pos_ref, freq_ref, gain_ref, gain2_ref, k_hbm, v_hbm, wq_hbm, wk_hbm, wv_hbm, wo_hbm,
                k_ref, v_ref, x1_ref, xn_ref, wq, wkv, wo, kbuf, vbuf, xs, qbuf, obuf, sbuf, knew, vnew,
                q_sem, kv_sem, o_sem, k_sem, v_sem):
    rows, width = x_ref.shape
    dim = wk_hbm.shape[1]
    heads = wq_hbm.shape[1] // dim
    ctx = k_hbm.shape[1]
    slots = kbuf.shape[0]
    groups = rows // group
    wide = wo.shape[2]
    n_out = wo.shape[0]

    def q_load(h):
        return pltpu.make_async_copy(wq_hbm.at[:, pl.ds(h * dim, dim)], wq.at[h], q_sem.at[h])

    def kv_load(i):
        return pltpu.make_async_copy((wk_hbm, wv_hbm)[i], wkv.at[i], kv_sem.at[i])

    def o_load(n):
        return pltpu.make_async_copy(wo_hbm.at[:, pl.ds(n * wide, wide)], wo.at[n], o_sem.at[n])

    def k_load(g):
        return pltpu.make_async_copy(k_hbm.at[pl.ds(g * group, group)], kbuf.at[lax.rem(g, slots)], k_sem.at[lax.rem(g, slots)])

    def v_load(g):
        return pltpu.make_async_copy(v_hbm.at[pl.ds(g * group, group)], vbuf.at[lax.rem(g, slots)], v_sem.at[lax.rem(g, slots)])

    kv_load(0).start()
    kv_load(1).start()
    for h in range(heads):
        q_load(h).start()
    for g in range(slots):
        k_load(g).start()
        v_load(g).start()
    for n in range(n_out):
        o_load(n).start()

    xw = x_ref[...].astype(jnp.float32)
    inv = lax.rsqrt(jnp.mean(xw * xw, axis=-1, keepdims=True) + 1e-6)
    xs[...] = (xw * inv * (1.0 + gain_ref[...].astype(jnp.float32))).astype(jnp.bfloat16)
    angle = pos_ref[...].astype(jnp.float32) * freq_ref[...]
    cos_t, sin_t = jnp.cos(angle), jnp.sin(angle)
    half = dim // 2

    def rotate(t):
        a, b = t[:, :half], t[:, half:]
        return a * cos_t - b * sin_t, b * cos_t + a * sin_t

    kv_load(0).wait()
    ka, kb = rotate(jnp.dot(xs[...], wkv[0], preferred_element_type=jnp.float32))
    ka, kb = ka.astype(jnp.bfloat16), kb.astype(jnp.bfloat16)
    k_ref[:, :half] = ka
    k_ref[:, half:] = kb
    knew[:, :half] = ka.astype(jnp.float32)
    knew[:, half:] = kb.astype(jnp.float32)
    kv_load(1).wait()
    vv = jnp.dot(xs[...], wkv[1], preferred_element_type=jnp.float32).astype(jnp.bfloat16)
    v_ref[...] = vv
    vnew[...] = vv.astype(jnp.float32)

    scale = dim ** -0.5
    for h in range(heads):
        q_load(h).wait()
        qa, qb = rotate(jnp.dot(xs[...], wq[h], preferred_element_type=jnp.float32))
        qbuf[0, pl.ds(h, rows, stride=heads), :] = (qa * scale).astype(jnp.bfloat16).astype(jnp.float32)
        qbuf[1, pl.ds(h, rows, stride=heads), :] = (qb * scale).astype(jnp.bfloat16).astype(jnp.float32)

    spots = lax.broadcasted_iota(jnp.int32, (heads, ctx), 1)

    def scores(g):
        k_load(g).wait()
        slot = lax.rem(g, slots)
        for i in range(group):
            spot = pl.ds(pl.multiple_of((g * group + i) * heads, heads), heads)
            q = jnp.concatenate([qbuf[0, spot, :], qbuf[1, spot, :]], axis=1).astype(jnp.bfloat16)
            sbuf[lax.rem(g, 2), i] = lax.dot_general(q, kbuf[slot, i], (((1,), (1,)), ((), ())), preferred_element_type=jnp.float32)

    def values(g):
        v_load(g).wait()
        slot = lax.rem(g, slots)
        for i in range(group):
            r = g * group + i
            spot = pl.ds(pl.multiple_of(r * heads, heads), heads)
            k_row = knew[pl.ds(r, 1), :]
            v_row = vnew[pl.ds(r, 1), :]
            new = jnp.sum(qbuf[0, spot, :] * k_row[:, :half] + qbuf[1, spot, :] * k_row[:, half:], axis=1, keepdims=True)
            valid = spots < len_ref[r]
            s = jnp.where(valid, sbuf[lax.rem(g, 2), i], -jnp.inf)
            peak = jnp.maximum(jnp.max(s, axis=1, keepdims=True), new)
            w = jnp.exp(s - peak)
            new_w = jnp.exp(new - peak)
            total = jnp.sum(w, axis=1, keepdims=True) + new_w
            prob = (w / total).astype(jnp.bfloat16)
            new_p = (new_w / total).astype(jnp.bfloat16).astype(jnp.float32)
            o = jnp.dot(prob, vbuf[slot, i], preferred_element_type=jnp.float32)
            o = o + new_p * v_row
            obuf[0, spot, :] = o[:, :half]
            obuf[1, spot, :] = o[:, half:]

    scores(0)
    k_load(slots).start()

    def body(g, carry):
        @pl.when(g + 1 < groups)
        def _():
            scores(g + 1)
        values(g)
        @pl.when(g + slots < groups)
        def _():
            v_load(g + slots).start()
        @pl.when(g + 1 + slots < groups)
        def _():
            k_load(g + 1 + slots).start()
        return carry
    lax.fori_loop(0, groups, body, 0)

    for h in range(heads):
        xs[:, h * dim:h * dim + half] = obuf[0, pl.ds(h, rows, stride=heads), :].astype(jnp.bfloat16)
        xs[:, h * dim + half:(h + 1) * dim] = obuf[1, pl.ds(h, rows, stride=heads), :].astype(jnp.bfloat16)

    def project(n, carry):
        o_load(n).wait()
        cols = pl.ds(pl.multiple_of(n * wide, wide), wide)
        x1_ref[:, cols] = x_ref[:, cols].astype(jnp.float32) + jnp.dot(xs[...], wo[n], preferred_element_type=jnp.float32)
        return carry
    lax.fori_loop(0, n_out, project, 0)
    x1 = x1_ref[...]
    inv = lax.rsqrt(jnp.mean(x1 * x1, axis=-1, keepdims=True) + 1e-6)
    xn_ref[...] = (x1 * inv * (1.0 + gain2_ref[...].astype(jnp.float32))).astype(jnp.bfloat16)


def attention(hidden_in, k_cache, v_cache, cache_len, norm_attn, norm_mlp, w_q, w_k, w_v, w_o):
    rows, width = hidden_in.shape
    ctx, dim = k_cache.shape[1:]
    heads = w_q.shape[1] // dim
    group, slots, wide = 8, 4, 512
    n_out = width // wide
    sems = pltpu.SemaphoreType.DMA
    vmem = pl.BlockSpec(memory_space=pltpu.VMEM)
    smem = pl.BlockSpec(memory_space=pltpu.SMEM)
    hbm = pl.BlockSpec(memory_space=pl.ANY)
    freq = 10000.0 ** (-2.0 * jnp.arange(dim // 2, dtype=jnp.float32) / dim)
    return pl.pallas_call(
        functools.partial(attn_kernel, group),
        out_shape=[jax.ShapeDtypeStruct((rows, dim), jnp.bfloat16)] * 2
        + [jax.ShapeDtypeStruct((rows, width), jnp.float32), jax.ShapeDtypeStruct((rows, width), jnp.bfloat16)],
        in_specs=[vmem, smem, vmem, vmem, vmem, vmem] + [hbm] * 6,
        out_specs=[vmem] * 4,
        scratch_shapes=[
            pltpu.VMEM((heads, width, dim), jnp.bfloat16),
            pltpu.VMEM((2, width, dim), jnp.bfloat16),
            pltpu.VMEM((n_out, heads * dim, wide), jnp.bfloat16),
            pltpu.VMEM((slots, group, ctx, dim), jnp.bfloat16),
            pltpu.VMEM((slots, group, ctx, dim), jnp.bfloat16),
            pltpu.VMEM((rows, width), jnp.bfloat16),
            pltpu.VMEM((2, rows * heads, dim // 2), jnp.float32),
            pltpu.VMEM((2, rows * heads, dim // 2), jnp.float32),
            pltpu.VMEM((2, group, heads, ctx), jnp.float32),
            pltpu.VMEM((rows, dim), jnp.float32),
            pltpu.VMEM((rows, dim), jnp.float32),
            sems((heads,)), sems((2,)), sems((n_out,)), sems((slots,)), sems((slots,)),
        ],
        compiler_params=pltpu.CompilerParams(vmem_limit_bytes=60 * 1024 * 1024),
        cost_estimate=pl.CostEstimate(flops=8 * rows * width * width, bytes_accessed=4 * rows * ctx * dim, transcendentals=0),
        name='attn',
    )(hidden_in, cache_len, cache_len[:, None], freq[None], norm_attn[None], norm_mlp[None], k_cache, v_cache, w_q, w_k, w_v, w_o)


def mlp_kernel(half, tile, depth_tile, xn_ref, x_ref, wg_hbm, wu_hbm, wd_hbm, out_ref,
               wg, wu, wd, xb, hid, own, snd, prt, ring,
               w_sem, ag_send, ag_recv, d_send, d_recv, r_send, r_recv):
    chips = lax.axis_size('tp') // 2
    me = lax.axis_index('tp')
    core = lax.rem(me, 2)
    chip = me // 2
    partner = me + 1 - 2 * core
    ahead = 2 * lax.rem(chip + 1, chips) + core
    behind = 2 * lax.rem(chip + chips - 1, chips) + core
    rows = 2 * half
    n_up = wg.shape[0]
    n_down = wd.shape[0]

    def to(src, dst, send, recv, dev):
        return pltpu.make_async_remote_copy(src_ref=src, dst_ref=dst, send_sem=send, recv_sem=recv,
                                            device_id={'tp': dev}, device_id_type=MESH)

    barrier = pltpu.get_barrier_semaphore()
    for dev in (partner, ahead, behind):
        pl.semaphore_signal(barrier, inc=1, device_id={'tp': dev}, device_id_type=MESH)

    def up_load(i, n):
        src, dst = ((wg_hbm, wg), (wu_hbm, wu))[i]
        return pltpu.make_async_copy(src.at[:, pl.ds(n * tile, tile)], dst.at[n], w_sem.at[i, n])

    def down_load(n):
        return pltpu.make_async_copy(wd_hbm.at[:, pl.ds(n * depth_tile, depth_tile)], wd.at[n], w_sem.at[2, n])

    for n in range(n_up):
        up_load(0, n).start()
        up_load(1, n).start()
    for n in range(n_down):
        down_load(n).start()

    lo, hi = pl.ds(0, half), pl.ds(half, half)
    mine, theirs = pl.ds(0, rows), pl.ds(rows, rows)
    pl.semaphore_wait(barrier, 3)

    gather = [
        to(xn_ref, xb.at[0, theirs], ag_send.at[0], ag_recv.at[0], partner),
        to(xn_ref.at[lo], xb.at[1, hi], ag_send.at[1], ag_recv.at[1], ahead),
        to(xn_ref.at[hi], xb.at[1, lo], ag_send.at[2], ag_recv.at[2], behind),
        to(xn_ref.at[hi], xb.at[2, hi], ag_send.at[3], ag_recv.at[3], ahead),
        to(xn_ref.at[lo], xb.at[2, lo], ag_send.at[4], ag_recv.at[4], behind),
        to(xb.at[1, hi], xb.at[3, lo], ag_send.at[5], ag_recv.at[5], ahead),
        to(xb.at[1, lo], xb.at[3, hi], ag_send.at[6], ag_recv.at[6], behind),
        to(xb.at[1, mine], xb.at[1, theirs], ag_send.at[7], ag_recv.at[7], partner),
        to(xb.at[2, mine], xb.at[2, theirs], ag_send.at[8], ag_recv.at[8], partner),
        to(xb.at[3, mine], xb.at[3, theirs], ag_send.at[9], ag_recv.at[9], partner),
    ]
    for copy in gather[:5]:
        copy.start()
    xb[0, 0:rows, :] = xn_ref[...]

    def up(b):
        def body(n, carry):
            if b == 0:
                up_load(0, n).wait()
                up_load(1, n).wait()
            gate = jnp.dot(xb[b], wg[n], preferred_element_type=jnp.float32)
            lin = jnp.dot(xb[b], wu[n], preferred_element_type=jnp.float32)
            act = jax.nn.gelu(gate, approximate=True) * lin
            hid[:, pl.ds(pl.multiple_of(n * tile, tile), tile)] = act.astype(jnp.bfloat16)
            return carry
        lax.fori_loop(0, n_up, body, 0, unroll=True)

    def exchange(b, n):
        return to(snd.at[b, n], prt.at[b, n], d_send.at[b, n], d_recv.at[b, n], partner)

    def hops(step, b, n):
        return (to(own.at[b, n, lo], ring.at[step, n, lo], r_send.at[step, 0, n], r_recv.at[step, 0, n], ahead),
                to(own.at[b, n, hi], ring.at[step, n, hi], r_send.at[step, 1, n], r_recv.at[step, 1, n], behind))

    def merge(b, n, step):
        exchange(b, n).wait_recv()
        own[b, n] = own[b, n] + prt[b, n]
        if step is not None:
            for copy in hops(step, b, n):
                copy.start()

    def down(b, step):
        def body(n, carry):
            if b == 0:
                down_load(n).wait()
            part = jnp.dot(hid[...], wd[n], preferred_element_type=jnp.float32)
            own[b, n] = part[0:rows]
            snd[b, n] = part[rows:2 * rows]
            exchange(b, n).start()
            @pl.when(n > 0)
            def _():
                merge(b, n - 1, step)
            return carry
        lax.fori_loop(0, n_down, body, 0, unroll=True)
        merge(b, n_down - 1, step)

    gather[0].wait_recv()
    up(0)
    down(0, None)
    gather[1].wait_recv()
    gather[2].wait_recv()
    gather[7].start()
    gather[5].start()
    gather[6].start()
    gather[7].wait_recv()
    up(1)
    gather[3].wait_recv()
    gather[4].wait_recv()
    gather[8].start()
    down(1, 0)
    gather[5].wait_recv()
    gather[6].wait_recv()
    gather[9].start()
    gather[9].wait_recv()
    up(3)
    down(3, 1)
    gather[8].wait_recv()
    up(2)
    down(2, None)

    def relay(n, carry):
        for copy in hops(1, 3, n):
            copy.wait_recv()
        own[2, n] = own[2, n] + ring[1, n]
        for copy in hops(2, 2, n):
            copy.start()
        for copy in hops(0, 1, n):
            copy.wait_recv()
        own[0, n, lo] = own[0, n, lo] + ring[0, n, hi]
        own[0, n, hi] = own[0, n, hi] + ring[0, n, lo]
        return carry
    lax.fori_loop(0, n_down, relay, 0)

    def finish(n, carry):
        for copy in hops(2, 2, n):
            copy.wait_recv()
        cols = pl.ds(pl.multiple_of(n * depth_tile, depth_tile), depth_tile)
        out_ref[:, cols] = (x_ref[:, cols] + (own[0, n] + ring[2, n])).astype(jnp.bfloat16)
        return carry
    lax.fori_loop(0, n_down, finish, 0)

    for copy in gather:
        copy.wait_send()
    def drain(n, carry):
        for b in range(4):
            exchange(b, n).wait_send()
        for step, b in ((0, 1), (1, 3), (2, 2)):
            for copy in hops(step, b, n):
                copy.wait_send()
        return carry
    lax.fori_loop(0, n_down, drain, 0)


def mlp(xn, x_mid, w_gate, w_up, w_down):
    rows, width = xn.shape
    units = w_gate.shape[1]
    tile = 512
    depth_tile = 512
    n_up, n_down = units // tile, width // depth_tile
    sems = pltpu.SemaphoreType.DMA
    vmem = pl.BlockSpec(memory_space=pltpu.VMEM)
    hbm = pl.BlockSpec(memory_space=pl.ANY)
    return pl.pallas_call(
        functools.partial(mlp_kernel, rows // 2, tile, depth_tile),
        out_shape=jax.ShapeDtypeStruct((rows, width), jnp.bfloat16),
        in_specs=[vmem, vmem, hbm, hbm, hbm],
        out_specs=vmem,
        scratch_shapes=[
            pltpu.VMEM((n_up, width, tile), jnp.bfloat16),
            pltpu.VMEM((n_up, width, tile), jnp.bfloat16),
            pltpu.VMEM((n_down, units, depth_tile), jnp.bfloat16),
            pltpu.VMEM((4, 2 * rows, width), jnp.bfloat16),
            pltpu.VMEM((2 * rows, units), jnp.bfloat16),
            pltpu.VMEM((4, n_down, rows, depth_tile), jnp.float32),
            pltpu.VMEM((4, n_down, rows, depth_tile), jnp.float32),
            pltpu.VMEM((4, n_down, rows, depth_tile), jnp.float32),
            pltpu.VMEM((3, n_down, rows, depth_tile), jnp.float32),
            sems((3, max(n_up, n_down))),
            sems((10,)), sems((10,)),
            sems((4, n_down)), sems((4, n_down)),
            sems((3, 2, n_down)), sems((3, 2, n_down)),
        ],
        compiler_params=pltpu.CompilerParams(collective_id=0, has_side_effects=True, vmem_limit_bytes=60 * 1024 * 1024),
        cost_estimate=pl.CostEstimate(flops=2 * 8 * rows * width * units * 3, bytes_accessed=6 * width * units, transcendentals=0),
        name='mlp',
    )(xn, x_mid, w_gate, w_up, w_down)


def solution(mesh):
    row_spec = P(('dp', 'tp'), None)
    cache_spec = P(('dp', 'tp'), None, None)
    full_vec = P(None)
    full_mat = P(None, None)

    def per_device(hidden_in, k_cache, v_cache, cache_len, norm_attn, norm_mlp, w_q, w_k, w_v, w_o, w_gate, w_up, w_down):
        k_new, v_new, x_mid, xn_mid = attention(hidden_in, k_cache, v_cache, cache_len, norm_attn, norm_mlp, w_q, w_k, w_v, w_o)
        return mlp(xn_mid, x_mid, w_gate, w_up, w_down), k_new, v_new

    return jax.shard_map(
        per_device,
        mesh=mesh,
        in_specs=(row_spec, cache_spec, cache_spec, P(('dp', 'tp')), full_vec, full_vec,
                  full_mat, full_mat, full_mat, full_mat, P(None, 'tp'), P(None, 'tp'), P('tp', None)),
        out_specs=(row_spec, row_spec, row_spec),
        check_vma=False,
    )
```

```python
import functools

import jax
import jax.numpy as jnp
import numpy as np
from jax import lax
from jax.experimental import pallas as pl
from jax.experimental.pallas import tpu as pltpu
from jax.sharding import PartitionSpec as P

MESH = pl.DeviceIdType.MESH


def layer_kernel(group, x_ref, len_ref, freq_ref, gain_ref, gain2_ref, k_hbm, v_hbm, wq_hbm, wk_hbm, wv_hbm, wo_hbm,
                 wg_hbm, wu_hbm, wd_hbm, out_ref, k_ref, v_ref,
                 wg, wu, wd, wkv, kbuf, vbuf, xs, qbuf, obuf, sbuf, knew, vnew, turn, x1, xb, hid, own, snd, prt, ring,
                 w_sem, q_sem, kv_sem, o_sem, k_sem, v_sem, ag_send, ag_recv, d_send, d_recv, r_send, r_recv):
    chips = lax.axis_size('tp') // 2
    me = lax.axis_index('tp')
    core = lax.rem(me, 2)
    chip = me // 2
    partner = me + 1 - 2 * core
    ahead = 2 * lax.rem(chip + 1, chips) + core
    behind = 2 * lax.rem(chip + chips - 1, chips) + core

    rows, width = x_ref.shape
    dim = wk_hbm.shape[1]
    heads = wq_hbm.shape[1] // dim
    ctx = k_hbm.shape[1]
    slots = kbuf.shape[0]
    groups = rows // group
    n_tile, _, tile = wg.shape
    side = rows // 2
    quart = rows // 4
    half = dim // 2
    per_part = groups // 2
    per_side = per_part // 2

    barrier = pltpu.get_barrier_semaphore()
    for dev in (partner, ahead, behind):
        pl.semaphore_signal(barrier, inc=1, device_id={'tp': dev}, device_id_type=MESH)

    def fetch(hbm, buf, n, sem):
        return pltpu.make_async_copy(hbm.at[:, pl.ds(pl.multiple_of(n * tile, tile), tile)], buf.at[n], sem)

    def q_load(n):
        return fetch(wq_hbm, wd, n, q_sem.at[n])

    def o_load(n):
        return fetch(wo_hbm, wu, n, o_sem.at[n])

    def gate_load(n):
        return fetch(wg_hbm, wg, n, w_sem.at[0, n])

    def up_load(n):
        return fetch(wu_hbm, wu, n, w_sem.at[1, n])

    def down_load(n):
        return fetch(wd_hbm, wd, n, w_sem.at[2, n])

    def kv_load(i):
        return pltpu.make_async_copy((wk_hbm, wv_hbm)[i], wkv.at[i], kv_sem.at[i])

    def first_row(g):
        j = lax.rem(g, per_part)
        return pl.multiple_of((j // per_side) * side + (g // per_part) * quart + lax.rem(j, per_side) * group, group)

    def k_load(g):
        slot = lax.rem(g, slots)
        return pltpu.make_async_copy(k_hbm.at[pl.ds(first_row(g), group)], kbuf.at[slot], k_sem.at[slot])

    def v_load(g):
        slot = lax.rem(g, slots)
        return pltpu.make_async_copy(v_hbm.at[pl.ds(first_row(g), group)], vbuf.at[slot], v_sem.at[slot])

    def to(src, dst, send, recv, dev):
        return pltpu.make_async_remote_copy(src_ref=src, dst_ref=dst, send_sem=send, recv_sem=recv,
                                            device_id={'tp': dev}, device_id_type=MESH)

    kv_load(0).start()
    kv_load(1).start()
    for n in range(n_tile):
        q_load(n).start()

    xw = x_ref[...].astype(jnp.float32)
    inv = lax.rsqrt(jnp.mean(xw * xw, axis=-1, keepdims=True) + 1e-6)
    xs[...] = (xw * inv * (1.0 + gain_ref[...].astype(jnp.float32)[None])).astype(jnp.bfloat16)
    for r in range(rows):
        turn[pl.ds(r, 1), :] = len_ref[r].astype(jnp.float32) * freq_ref[...]
    angle = turn[...]
    cos_t, sin_t = jnp.cos(angle), jnp.sin(angle)

    def rotate(a, b):
        return a * cos_t - b * sin_t, b * cos_t + a * sin_t

    kv_load(0).wait()
    kk = jnp.dot(xs[...], wkv[0], preferred_element_type=jnp.float32)
    ka, kb = rotate(kk[:, :half], kk[:, half:])
    ka, kb = ka.astype(jnp.bfloat16), kb.astype(jnp.bfloat16)
    k_ref[:, :half] = ka
    k_ref[:, half:] = kb
    knew[:, :half] = ka.astype(jnp.float32)
    knew[:, half:] = kb.astype(jnp.float32)
    kv_load(1).wait()
    vv = jnp.dot(xs[...], wkv[1], preferred_element_type=jnp.float32).astype(jnp.bfloat16)
    v_ref[...] = vv
    vnew[...] = vv.astype(jnp.float32)

    scale = dim ** -0.5
    for n in range(n_tile):
        q_load(n).wait()
        if n < slots:
            k_load(n).start()
            v_load(n).start()
        ql = jnp.dot(xs[...], wd[n], preferred_element_type=jnp.float32)
        for i in range(tile // dim):
            h = n * (tile // dim) + i
            qa, qb = rotate(ql[:, i * dim:i * dim + half], ql[:, i * dim + half:(i + 1) * dim])
            qbuf[0, pl.ds(h, rows, stride=heads), :] = (qa * scale).astype(jnp.bfloat16).astype(jnp.float32)
            qbuf[1, pl.ds(h, rows, stride=heads), :] = (qb * scale).astype(jnp.bfloat16).astype(jnp.float32)
    for n in range(n_tile):
        o_load(n).start()

    spots = lax.broadcasted_iota(jnp.int32, (heads, ctx), 1)

    def scores(g):
        slot = lax.rem(g, slots)
        base = first_row(lax.rem(g, groups))
        for i in range(group):
            spot = pl.ds(pl.multiple_of((base + i) * heads, heads), heads)
            q = jnp.concatenate([qbuf[0, spot, :], qbuf[1, spot, :]], axis=1).astype(jnp.bfloat16)
            sbuf[lax.rem(g, 2), i] = lax.dot_general(q, kbuf[slot, i], (((1,), (1,)), ((), ())), preferred_element_type=jnp.float32)

    def values(g):
        slot = lax.rem(g, slots)
        base = first_row(g)
        for i in range(group):
            r = base + i
            spot = pl.ds(pl.multiple_of(r * heads, heads), heads)
            k_row = knew[pl.ds(r, 1), :]
            v_row = vnew[pl.ds(r, 1), :]
            new = jnp.sum(qbuf[0, spot, :] * k_row[:, :half] + qbuf[1, spot, :] * k_row[:, half:], axis=1, keepdims=True)
            valid = spots < len_ref[r]
            s = jnp.where(valid, sbuf[lax.rem(g, 2), i], -jnp.inf)
            peak = jnp.maximum(jnp.max(s, axis=1, keepdims=True), new)
            w = jnp.exp(s - peak)
            new_w = jnp.exp(new - peak)
            total = jnp.sum(w, axis=1, keepdims=True) + new_w
            prob = (w / total).astype(jnp.bfloat16)
            new_p = (new_w / total).astype(jnp.bfloat16).astype(jnp.float32)
            o = jnp.dot(prob, vbuf[slot, i], preferred_element_type=jnp.float32) + new_p * v_row
            to_spot = pl.ds(pl.multiple_of((lax.rem(g, per_part) * group + i) * heads, heads), heads)
            obuf[0, to_spot, :] = o[:, :half]
            obuf[1, to_spot, :] = o[:, half:]

    def attend(g, carry):
        @pl.when(g + 1 < groups)
        def _():
            k_load(g + 1).wait()
        v_load(g).wait()
        scores(g + 1)
        values(g)
        @pl.when(g + slots < groups)
        def _():
            v_load(g + slots).start()
        @pl.when(g + 1 + slots < groups)
        def _():
            k_load(g + 1 + slots).start()
        @pl.when(g >= groups - n_tile)
        def _():
            gate_load(g - (groups - n_tile)).start()
        return carry

    def finish(s):
        for h in range(heads):
            spot = pl.ds(h, side, stride=heads)
            xs[0:side, h * dim:h * dim + half] = obuf[0, spot, :].astype(jnp.bfloat16)
            xs[0:side, h * dim + half:(h + 1) * dim] = obuf[1, spot, :].astype(jnp.bfloat16)
        a, b = pl.ds(s * quart, quart), pl.ds(side + s * quart, quart)

        def project(n, carry):
            if s == 0:
                o_load(n).wait()
            cols = pl.ds(pl.multiple_of(n * tile, tile), tile)
            mixed = jnp.dot(xs[0:side, :], wu[n], preferred_element_type=jnp.float32)
            x1[a, cols] = x_ref[a, cols].astype(jnp.float32) + mixed[0:quart]
            x1[b, cols] = x_ref[b, cols].astype(jnp.float32) + mixed[quart:side]
            if s == 1:
                up_load(n).start()
            return carry
        lax.fori_loop(0, n_tile, project, 0)
        for j, part in ((0, a), (1, b)):
            mid = x1[part, :]
            inv = lax.rsqrt(jnp.mean(mid * mid, axis=-1, keepdims=True) + 1e-6)
            normed = (mid * inv * (1.0 + gain2_ref[...].astype(jnp.float32)[None])).astype(jnp.bfloat16)
            xb[2 * s + 1, side + j * quart:side + (j + 1) * quart, :] = normed

    def span(i, n=1):
        return pl.ds(i * quart, n * quart)

    def gather(s, i):
        near, far = 2 * s, 2 * s + 1
        src, dst, dev = (
            (xb.at[far, span(2)], xb.at[near, span(1)], ahead),
            (xb.at[far, span(3)], xb.at[near, span(3)], ahead),
            (xb.at[far, span(3)], xb.at[near, span(0)], behind),
            (xb.at[far, span(2)], xb.at[near, span(2)], behind),
            (xb.at[near, span(1)], xb.at[far, span(0)], ahead),
            (xb.at[near, span(0)], xb.at[far, span(1)], behind),
            (xb.at[near, span(0, 2)], xb.at[near, span(4, 2)], partner),
            (xb.at[near, span(2, 2)], xb.at[near, span(6, 2)], partner),
            (xb.at[far, span(0, 4)], xb.at[far, span(4, 4)], partner),
        )[i]
        return to(src, dst, ag_send.at[s, i], ag_recv.at[s, i], dev)

    def send(s):
        for i in (0, 2, 1, 3):
            gather(s, i).start()

    def arrive(s, *ids):
        for i in ids:
            gather(s, i).wait_recv()

    def forward(s):
        arrive(s, 0, 2)
        for i in (4, 5, 6):
            gather(s, i).start()

    k_load(0).wait()
    scores(0)
    k_load(slots).start()
    lax.fori_loop(0, per_part, attend, 0)
    finish(0)
    pl.semaphore_wait(barrier, 3)
    send(0)
    lax.fori_loop(per_part, groups, attend, 0)
    forward(0)
    finish(1)
    for n in range(n_tile):
        down_load(n).start()
    send(1)

    def up_step(b, n):
        if b == 0:
            gate_load(n).wait()
            up_load(n).wait()
        gate = jnp.dot(xb[b], wg[n], preferred_element_type=jnp.float32)
        lin = jnp.dot(xb[b], wu[n], preferred_element_type=jnp.float32)
        hid[:, n * tile:(n + 1) * tile] = (jax.nn.gelu(gate, approximate=True) * lin).astype(jnp.bfloat16)

    def swap(b, n):
        return to(snd.at[b, n], prt.at[b, n], d_send.at[b, n], d_recv.at[b, n], partner)

    def hops(s, step, n):
        b = (2 * s, 2 * s + 1, 2 * s)[step]
        fwd = (0, 0, 2)[step]
        return (to(own.at[b, n, span(fwd)], ring.at[s, step, n, span(0)], r_send.at[s, step, 0, n], r_recv.at[s, step, 0, n], ahead),
                to(own.at[b, n, span(fwd + 1)], ring.at[s, step, n, span(1)], r_send.at[s, step, 1, n], r_recv.at[s, step, 1, n], behind))

    def merge(b, n):
        swap(b, n).wait_recv()
        own[b, n] = own[b, n] + prt[b, n]
        for copy in hops(b // 2, b % 2, n):
            copy.start()

    def down(b):
        for n in range(n_tile):
            if b == 0:
                down_load(n).wait()
            part = jnp.dot(hid[...], wd[n], preferred_element_type=jnp.float32)
            own[b, n] = part[0:rows]
            snd[b, n] = part[rows:2 * rows]
            swap(b, n).start()
            if n > 0:
                merge(b, n - 1)
        merge(b, n_tile - 1)

    def relay(s, n):
        for copy in hops(s, 1, n):
            copy.wait_recv()
        own[2 * s, n, span(2, 2)] = own[2 * s, n, span(2, 2)] + ring[s, 1, n]
        for copy in hops(s, 2, n):
            copy.start()

    def settle(s, n):
        for step in (0, 2):
            for copy in hops(s, step, n):
                copy.wait_recv()
        cols = slice(n * tile, (n + 1) * tile)
        a, b = pl.ds(s * quart, quart), pl.ds(side + s * quart, quart)
        far = 2 * s + 1
        out_ref[a, cols] = (x1[a, cols] + (own[far, n, span(2)] + (ring[s, 0, n, span(1)] + ring[s, 2, n, span(0)]))).astype(jnp.bfloat16)
        out_ref[b, cols] = (x1[b, cols] + (own[far, n, span(3)] + (ring[s, 0, n, span(0)] + ring[s, 2, n, span(1)]))).astype(jnp.bfloat16)

    arrive(0, 1, 3)
    gather(0, 7).start()
    arrive(0, 6, 7)
    for n in range(n_tile):
        up_step(0, n)
    forward(1)
    arrive(0, 4, 5)
    gather(0, 8).start()
    down(0)
    arrive(1, 1, 3)
    gather(1, 7).start()
    arrive(0, 8)
    for n in range(n_tile):
        up_step(1, n)
    down(1)
    arrive(1, 4, 5)
    gather(1, 8).start()
    arrive(1, 6, 7)
    for n in range(n_tile):
        up_step(2, n)
        relay(0, n)
    down(2)
    arrive(1, 8)
    for n in range(n_tile):
        up_step(3, n)
    down(3)
    for n in range(n_tile):
        settle(0, n)
    for n in range(n_tile):
        relay(1, n)
    for n in range(n_tile):
        settle(1, n)

    for s in range(2):
        for i in range(9):
            gather(s, i).wait_send()

    def drain(n, carry):
        for b in range(4):
            swap(b, n).wait_send()
        for s in range(2):
            for step in range(3):
                for copy in hops(s, step, n):
                    copy.wait_send()
        return carry
    lax.fori_loop(0, n_tile, drain, 0)


def layer(hidden_in, k_cache, v_cache, cache_len, norm_attn, norm_mlp, w_q, w_k, w_v, w_o, w_gate, w_up, w_down):
    rows, width = hidden_in.shape
    ctx, dim = k_cache.shape[1:]
    heads = w_q.shape[1] // dim
    units = w_gate.shape[1]
    group, slots, tile = 8, 4, 512
    n_tile = width // tile
    assert heads * dim == width and units == width
    sems = pltpu.SemaphoreType.DMA
    bf16, f32 = jnp.bfloat16, jnp.float32
    vmem = pl.BlockSpec(memory_space=pltpu.VMEM)
    smem = pl.BlockSpec(memory_space=pltpu.SMEM)
    hbm = pl.BlockSpec(memory_space=pl.ANY)
    freq = np.float32(10000.0 ** (-2.0 * np.arange(dim // 2) / dim))[None]
    return pl.pallas_call(
        functools.partial(layer_kernel, group),
        out_shape=[jax.ShapeDtypeStruct((rows, width), bf16)] + [jax.ShapeDtypeStruct((rows, dim), bf16)] * 2,
        in_specs=[vmem, smem, vmem, vmem, vmem] + [hbm] * 9,
        out_specs=[vmem] * 3,
        scratch_shapes=[
            pltpu.VMEM((n_tile, width, tile), bf16),
            pltpu.VMEM((n_tile, width, tile), bf16),
            pltpu.VMEM((n_tile, units, tile), bf16),
            pltpu.VMEM((2, width, dim), bf16),
            pltpu.VMEM((slots, group, ctx, dim), bf16),
            pltpu.VMEM((slots, group, ctx, dim), bf16),
            pltpu.VMEM((rows, width), bf16),
            pltpu.VMEM((2, rows * heads, dim // 2), f32),
            pltpu.VMEM((2, rows * heads // 2, dim // 2), f32),
            pltpu.VMEM((2, group, heads, ctx), f32),
            pltpu.VMEM((rows, dim), f32),
            pltpu.VMEM((rows, dim), f32),
            pltpu.VMEM((rows, dim // 2), f32),
            pltpu.VMEM((rows, width), f32),
            pltpu.VMEM((4, 2 * rows, width), bf16),
            pltpu.VMEM((2 * rows, units), bf16),
            pltpu.VMEM((4, n_tile, rows, tile), f32),
            pltpu.VMEM((4, n_tile, rows, tile), f32),
            pltpu.VMEM((4, n_tile, rows, tile), f32),
            pltpu.VMEM((2, 3, n_tile, rows // 2, tile), f32),
            sems((3, n_tile)), sems((n_tile,)), sems((2,)), sems((n_tile,)), sems((slots,)), sems((slots,)),
            sems((2, 9)), sems((2, 9)),
            sems((4, n_tile)), sems((4, n_tile)),
            sems((2, 3, 2, n_tile)), sems((2, 3, 2, n_tile)),
        ],
        compiler_params=pltpu.CompilerParams(collective_id=0, has_side_effects=True, vmem_limit_bytes=63 * 1024 * 1024),
        cost_estimate=pl.CostEstimate(flops=48 * rows * width * units, bytes_accessed=4 * rows * ctx * dim + 10 * width * width, transcendentals=0),
        name='layer',
    )(hidden_in, cache_len, freq, norm_attn, norm_mlp, k_cache, v_cache, w_q, w_k, w_v, w_o, w_gate, w_up, w_down)


def solution(mesh):
    row_spec = P(('dp', 'tp'), None)
    cache_spec = P(('dp', 'tp'), None, None)
    full_vec = P(None)
    full_mat = P(None, None)

    return jax.shard_map(
        layer,
        mesh=mesh,
        in_specs=(row_spec, cache_spec, cache_spec, P(('dp', 'tp')), full_vec, full_vec,
                  full_mat, full_mat, full_mat, full_mat, P(None, 'tp'), P(None, 'tp'), P('tp', None)),
        out_specs=(row_spec, row_spec, row_spec),
        check_vma=False,
    )
```

```python
import functools

import jax
import jax.numpy as jnp
import numpy as np
from jax import lax
from jax.experimental import pallas as pl
from jax.experimental.pallas import tpu as pltpu
from jax.sharding import PartitionSpec as P

MESH = pl.DeviceIdType.MESH


def layer_kernel(group, x_hbm, len_hbm, freq_hbm, gain_hbm, gain2_hbm, k_hbm, v_hbm, wq_hbm, wk_hbm, wv_hbm, wo_hbm,
                 wg_hbm, wu_hbm, wd_hbm, out_hbm, k_out, v_out,
                 x_ref, len_ref, freq_ref, gain_ref, gain2_ref, out_ref, k_ref, v_ref, wg, wu, wd, wkv, kbuf, vbuf, xs, qbuf, obuf, sbuf, knew, vnew, turn, x1, xb, hid, own, snd, prt, ring,
                 x_sem, y_sem, w_sem, q_sem, kv_sem, o_sem, k_sem, v_sem, ag_send, ag_recv, d_send, d_recv, r_send, r_recv):
    chips = lax.axis_size('tp') // 2
    me = lax.axis_index('tp')
    core = lax.rem(me, 2)
    chip = me // 2
    partner = me + 1 - 2 * core
    ahead = 2 * lax.rem(chip + 1, chips) + core
    behind = 2 * lax.rem(chip + chips - 1, chips) + core

    rows, width = x_ref.shape
    dim = wk_hbm.shape[1]
    heads = wq_hbm.shape[1] // dim
    ctx = k_hbm.shape[1]
    slots = kbuf.shape[0]
    groups = rows // group
    n_tile, _, tile = wg.shape
    side = rows // 2
    quart = rows // 4
    half = dim // 2
    per_part = groups // 2
    per_side = per_part // 2

    barrier = pltpu.get_barrier_semaphore()
    for dev in (partner, ahead, behind):
        pl.semaphore_signal(barrier, inc=1, device_id={'tp': dev}, device_id_type=MESH)

    def fetch(hbm, buf, n, sem):
        return pltpu.make_async_copy(hbm.at[:, pl.ds(pl.multiple_of(n * tile, tile), tile)], buf.at[n], sem)

    def q_load(n):
        return fetch(wq_hbm, wd, n, q_sem.at[n])

    def o_load(n):
        return fetch(wo_hbm, wu, n, o_sem.at[n])

    def gate_load(n):
        return fetch(wg_hbm, wg, n, w_sem.at[0, n])

    def up_load(n):
        return fetch(wu_hbm, wu, n, w_sem.at[1, n])

    def down_load(n):
        return fetch(wd_hbm, wd, n, w_sem.at[2, n])

    def kv_load(i):
        return pltpu.make_async_copy((wk_hbm, wv_hbm)[i], wkv.at[i], kv_sem.at[i])

    def first_row(g):
        j = lax.rem(g, per_part)
        return pl.multiple_of((j // per_side) * side + (g // per_part) * quart + lax.rem(j, per_side) * group, group)

    def k_load(g):
        slot = lax.rem(g, slots)
        return pltpu.make_async_copy(k_hbm.at[pl.ds(first_row(g), group)], kbuf.at[slot], k_sem.at[slot])

    def v_load(g):
        slot = lax.rem(g, slots)
        return pltpu.make_async_copy(v_hbm.at[pl.ds(first_row(g), group)], vbuf.at[slot], v_sem.at[slot])

    def to(src, dst, send, recv, dev):
        return pltpu.make_async_remote_copy(src_ref=src, dst_ref=dst, send_sem=send, recv_sem=recv,
                                            device_id={'tp': dev}, device_id_type=MESH)

    small = [pltpu.make_async_copy(src, dst, x_sem.at[i]) for i, (src, dst) in enumerate(
        ((x_hbm, x_ref), (gain_hbm, gain_ref), (len_hbm, len_ref), (freq_hbm, freq_ref), (gain2_hbm, gain2_ref)))]
    for copy in small:
        copy.start()
    kv_load(0).start()
    kv_load(1).start()
    for n in range(n_tile):
        q_load(n).start()
    for g in range(slots):
        k_load(g).start()
        v_load(g).start()

    for copy in small:
        copy.wait()
    xw = x_ref[...].astype(jnp.float32)
    inv = lax.rsqrt(jnp.mean(xw * xw, axis=-1, keepdims=True) + 1e-6)
    xs[...] = (xw * inv * (1.0 + gain_ref[...].astype(jnp.float32)[None])).astype(jnp.bfloat16)
    for r in range(rows):
        turn[pl.ds(r, 1), :] = len_ref[r].astype(jnp.float32) * freq_ref[...]
    angle = turn[...]
    cos_t, sin_t = jnp.cos(angle), jnp.sin(angle)

    def rotate(a, b):
        return a * cos_t - b * sin_t, b * cos_t + a * sin_t

    kv_load(0).wait()
    kk = jnp.dot(xs[...], wkv[0], preferred_element_type=jnp.float32)
    ka, kb = rotate(kk[:, :half], kk[:, half:])
    ka, kb = ka.astype(jnp.bfloat16), kb.astype(jnp.bfloat16)
    k_ref[:, :half] = ka
    k_ref[:, half:] = kb
    knew[:, :half] = ka.astype(jnp.float32)
    knew[:, half:] = kb.astype(jnp.float32)
    kv_load(1).wait()
    vv = jnp.dot(xs[...], wkv[1], preferred_element_type=jnp.float32).astype(jnp.bfloat16)
    v_ref[...] = vv
    vnew[...] = vv.astype(jnp.float32)
    outs = [pltpu.make_async_copy(k_ref, k_out, y_sem.at[0]), pltpu.make_async_copy(v_ref, v_out, y_sem.at[1])]
    for copy in outs:
        copy.start()

    scale = dim ** -0.5
    for n in range(n_tile):
        q_load(n).wait()
        ql = jnp.dot(xs[...], wd[n], preferred_element_type=jnp.float32)
        for i in range(tile // dim):
            h = n * (tile // dim) + i
            qa, qb = rotate(ql[:, i * dim:i * dim + half], ql[:, i * dim + half:(i + 1) * dim])
            qbuf[0, pl.ds(h, rows, stride=heads), :] = (qa * scale).astype(jnp.bfloat16).astype(jnp.float32)
            qbuf[1, pl.ds(h, rows, stride=heads), :] = (qb * scale).astype(jnp.bfloat16).astype(jnp.float32)

    spots = lax.broadcasted_iota(jnp.int32, (heads, ctx), 1)

    def scores(g):
        slot = lax.rem(g, slots)
        base = first_row(lax.rem(g, groups))
        for i in range(group):
            spot = pl.ds(pl.multiple_of((base + i) * heads, heads), heads)
            q = jnp.concatenate([qbuf[0, spot, :], qbuf[1, spot, :]], axis=1).astype(jnp.bfloat16)
            sbuf[lax.rem(g, 2), i] = lax.dot_general(q, kbuf[slot, i], (((1,), (1,)), ((), ())), preferred_element_type=jnp.float32)

    def values(g):
        slot = lax.rem(g, slots)
        base = first_row(g)
        for i in range(group):
            r = base + i
            spot = pl.ds(pl.multiple_of(r * heads, heads), heads)
            k_row = knew[pl.ds(r, 1), :]
            v_row = vnew[pl.ds(r, 1), :]
            new = jnp.sum(qbuf[0, spot, :] * k_row[:, :half] + qbuf[1, spot, :] * k_row[:, half:], axis=1, keepdims=True)
            valid = spots < len_ref[r]
            s = jnp.where(valid, sbuf[lax.rem(g, 2), i], -jnp.inf)
            peak = jnp.maximum(jnp.max(s, axis=1, keepdims=True), new)
            w = jnp.exp(s - peak)
            new_w = jnp.exp(new - peak)
            total = jnp.sum(w, axis=1, keepdims=True) + new_w
            prob = (w / total).astype(jnp.bfloat16)
            new_p = (new_w / total).astype(jnp.bfloat16).astype(jnp.float32)
            o = jnp.dot(prob, vbuf[slot, i], preferred_element_type=jnp.float32) + new_p * v_row
            to_spot = pl.ds(pl.multiple_of((lax.rem(g, per_part) * group + i) * heads, heads), heads)
            obuf[0, to_spot, :] = o[:, :half]
            obuf[1, to_spot, :] = o[:, half:]

    def attend(g, carry):
        @pl.when(g + 1 < groups)
        def _():
            k_load(g + 1).wait()
        v_load(g).wait()
        scores(g + 1)
        values(g)
        @pl.when(g + slots < groups)
        def _():
            v_load(g + slots).start()
        @pl.when(g + 1 + slots < groups)
        def _():
            k_load(g + 1 + slots).start()
        @pl.when(g < n_tile)
        def _():
            o_load(g).start()
        @pl.when(g >= groups - n_tile)
        def _():
            gate_load(g - (groups - n_tile)).start()
        return carry

    def finish(s):
        for h in range(heads):
            spot = pl.ds(h, side, stride=heads)
            xs[0:side, h * dim:h * dim + half] = obuf[0, spot, :].astype(jnp.bfloat16)
            xs[0:side, h * dim + half:(h + 1) * dim] = obuf[1, spot, :].astype(jnp.bfloat16)
        a, b = pl.ds(s * quart, quart), pl.ds(side + s * quart, quart)

        def project(n, carry):
            if s == 0:
                o_load(n).wait()
            cols = pl.ds(pl.multiple_of(n * tile, tile), tile)
            mixed = jnp.dot(xs[0:side, :], wu[n], preferred_element_type=jnp.float32)
            x1[a, cols] = x_ref[a, cols].astype(jnp.float32) + mixed[0:quart]
            x1[b, cols] = x_ref[b, cols].astype(jnp.float32) + mixed[quart:side]
            if s == 1:
                up_load(n).start()
            return carry
        lax.fori_loop(0, n_tile, project, 0)
        if s == 1:
            arrive(0, 1, 3)
            gather(0, 7).start()
        for j, part in ((0, a), (1, b)):
            mid = x1[part, :]
            inv = lax.rsqrt(jnp.mean(mid * mid, axis=-1, keepdims=True) + 1e-6)
            normed = (mid * inv * (1.0 + gain2_ref[...].astype(jnp.float32)[None])).astype(jnp.bfloat16)
            xb[2 * s + 1, side + j * quart:side + (j + 1) * quart, :] = normed

    def span(i, n=1):
        return pl.ds(i * quart, n * quart)

    def gather(s, i):
        near, far = 2 * s, 2 * s + 1
        src, dst, dev = (
            (xb.at[far, span(2)], xb.at[near, span(1)], ahead),
            (xb.at[far, span(3)], xb.at[near, span(3)], ahead),
            (xb.at[far, span(3)], xb.at[near, span(0)], behind),
            (xb.at[far, span(2)], xb.at[near, span(2)], behind),
            (xb.at[near, span(1)], xb.at[far, span(0)], ahead),
            (xb.at[near, span(0)], xb.at[far, span(1)], behind),
            (xb.at[near, span(0, 2)], xb.at[near, span(4, 2)], partner),
            (xb.at[near, span(2, 2)], xb.at[near, span(6, 2)], partner),
            (xb.at[far, span(0, 4)], xb.at[far, span(4, 4)], partner),
        )[i]
        return to(src, dst, ag_send.at[s, i], ag_recv.at[s, i], dev)

    def send(s):
        for i in (0, 2, 1, 3):
            gather(s, i).start()

    def arrive(s, *ids):
        for i in ids:
            gather(s, i).wait_recv()

    def forward(s):
        arrive(s, 0, 2)
        for i in (4, 5, 6):
            gather(s, i).start()

    k_load(0).wait()
    scores(0)
    k_load(slots).start()
    lax.fori_loop(0, per_part, attend, 0)
    finish(0)
    pl.semaphore_wait(barrier, 3)
    send(0)
    lax.fori_loop(per_part, groups, attend, 0)
    forward(0)
    finish(1)
    for n in range(n_tile):
        down_load(n).start()
    send(1)

    def up_step(b, n):
        if b == 0:
            gate_load(n).wait()
            up_load(n).wait()
        gate = jnp.dot(xb[b], wg[n], preferred_element_type=jnp.float32)
        lin = jnp.dot(xb[b], wu[n], preferred_element_type=jnp.float32)
        hid[:, n * tile:(n + 1) * tile] = (jax.nn.gelu(gate, approximate=True) * lin).astype(jnp.bfloat16)

    def swap(b, n):
        return to(snd.at[b, n], prt.at[b, n], d_send.at[b, n], d_recv.at[b, n], partner)

    def hops(s, step, n):
        b = (2 * s, 2 * s + 1, 2 * s)[step]
        fwd = (0, 0, 2)[step]
        return (to(own.at[b, n, span(fwd)], ring.at[s, step, n, span(0)], r_send.at[s, step, 0, n], r_recv.at[s, step, 0, n], ahead),
                to(own.at[b, n, span(fwd + 1)], ring.at[s, step, n, span(1)], r_send.at[s, step, 1, n], r_recv.at[s, step, 1, n], behind))

    def merge(b, n):
        swap(b, n).wait_recv()
        own[b, n] = own[b, n] + prt[b, n]
        for copy in hops(b // 2, b % 2, n):
            copy.start()

    pending = []

    def flush(keep=0):
        while len(pending) > keep:
            merge(*pending.pop(0))

    def up(b, after=None):
        for n in range(n_tile):
            up_step(b, n)
            flush()
            if after is not None:
                after(n)

    def down(b):
        for n in range(n_tile):
            if b == 0:
                down_load(n).wait()
            part = jnp.dot(hid[...], wd[n], preferred_element_type=jnp.float32)
            own[b, n] = part[0:rows]
            snd[b, n] = part[rows:2 * rows]
            swap(b, n).start()
            pending.append((b, n))
            flush(2)

    def relay(s, n):
        for copy in hops(s, 1, n):
            copy.wait_recv()
        own[2 * s, n, span(2, 2)] = own[2 * s, n, span(2, 2)] + ring[s, 1, n]
        for copy in hops(s, 2, n):
            copy.start()

    def settle(s, n):
        for step in (0, 2):
            for copy in hops(s, step, n):
                copy.wait_recv()
        cols = slice(n * tile, (n + 1) * tile)
        a, b = pl.ds(s * quart, quart), pl.ds(side + s * quart, quart)
        far = 2 * s + 1
        out_ref[a, cols] = (x1[a, cols] + (own[far, n, span(2)] + (ring[s, 0, n, span(1)] + ring[s, 2, n, span(0)]))).astype(jnp.bfloat16)
        out_ref[b, cols] = (x1[b, cols] + (own[far, n, span(3)] + (ring[s, 0, n, span(0)] + ring[s, 2, n, span(1)]))).astype(jnp.bfloat16)

    def give(s):
        a, b = pl.ds(s * quart, quart), pl.ds(side + s * quart, quart)
        for j, part in enumerate((a, b)):
            copy = pltpu.make_async_copy(out_ref.at[part], out_hbm.at[part], y_sem.at[2 + 2 * s + j])
            copy.start()
            outs.append(copy)

    arrive(0, 6, 7)
    up(0)
    forward(1)
    arrive(0, 4, 5)
    gather(0, 8).start()
    down(0)
    arrive(1, 1, 3)
    gather(1, 7).start()
    arrive(0, 8)
    up(1)
    down(1)
    arrive(1, 4, 5)
    gather(1, 8).start()
    arrive(1, 6, 7)
    up(2, lambda n: relay(0, n))
    down(2)
    arrive(1, 8)
    up(3)
    down(3)
    settle(0, 0)
    settle(0, 1)
    flush()
    for n in range(2, n_tile):
        settle(0, n)
    give(0)
    for n in range(n_tile):
        relay(1, n)
    for n in range(n_tile):
        settle(1, n)
    give(1)

    for s in range(2):
        for i in range(9):
            gather(s, i).wait_send()

    def drain(n, carry):
        for b in range(4):
            swap(b, n).wait_send()
        for s in range(2):
            for step in range(3):
                for copy in hops(s, step, n):
                    copy.wait_send()
        return carry
    lax.fori_loop(0, n_tile, drain, 0)
    for copy in outs:
        copy.wait()


def layer(hidden_in, k_cache, v_cache, cache_len, norm_attn, norm_mlp, w_q, w_k, w_v, w_o, w_gate, w_up, w_down):
    rows, width = hidden_in.shape
    ctx, dim = k_cache.shape[1:]
    heads = w_q.shape[1] // dim
    units = w_gate.shape[1]
    group, slots, tile = 8, 4, 512
    n_tile = width // tile
    assert heads * dim == width and units == width
    sems = pltpu.SemaphoreType.DMA
    bf16, f32 = jnp.bfloat16, jnp.float32
    hbm = pl.BlockSpec(memory_space=pl.ANY)
    freq = np.float32(10000.0 ** (-2.0 * np.arange(dim // 2) / dim))[None]
    results = pl.pallas_call(
        functools.partial(layer_kernel, group),
        out_shape=[jax.ShapeDtypeStruct((rows, width), bf16)] + [jax.ShapeDtypeStruct((rows, dim), bf16)] * 2,
        in_specs=[hbm] * 14,
        out_specs=[hbm] * 3,
        scratch_shapes=[
            pltpu.VMEM((rows, width), bf16),
            pltpu.SMEM((rows,), jnp.int32),
            pltpu.VMEM((1, dim // 2), f32),
            pltpu.VMEM((width,), bf16),
            pltpu.VMEM((width,), bf16),
            pltpu.VMEM((rows, width), bf16),
            pltpu.VMEM((rows, dim), bf16),
            pltpu.VMEM((rows, dim), bf16),
            pltpu.VMEM((n_tile, width, tile), bf16),
            pltpu.VMEM((n_tile, width, tile), bf16),
            pltpu.VMEM((n_tile, units, tile), bf16),
            pltpu.VMEM((2, width, dim), bf16),
            pltpu.VMEM((slots, group, ctx, dim), bf16),
            pltpu.VMEM((slots, group, ctx, dim), bf16),
            pltpu.VMEM((rows, width), bf16),
            pltpu.VMEM((2, rows * heads, dim // 2), f32),
            pltpu.VMEM((2, rows * heads // 2, dim // 2), f32),
            pltpu.VMEM((2, group, heads, ctx), f32),
            pltpu.VMEM((rows, dim), f32),
            pltpu.VMEM((rows, dim), f32),
            pltpu.VMEM((rows, dim // 2), f32),
            pltpu.VMEM((rows, width), f32),
            pltpu.VMEM((4, 2 * rows, width), bf16),
            pltpu.VMEM((2 * rows, units), bf16),
            pltpu.VMEM((4, n_tile, rows, tile), f32),
            pltpu.VMEM((4, n_tile, rows, tile), f32),
            pltpu.VMEM((4, n_tile, rows, tile), f32),
            pltpu.VMEM((2, 3, n_tile, rows // 2, tile), f32),
            sems((5,)), sems((6,)), sems((3, n_tile)), sems((n_tile,)), sems((2,)), sems((n_tile,)), sems((slots,)), sems((slots,)),
            sems((2, 9)), sems((2, 9)),
            sems((4, n_tile)), sems((4, n_tile)),
            sems((2, 3, 2, n_tile)), sems((2, 3, 2, n_tile)),
        ],
        compiler_params=pltpu.CompilerParams(collective_id=0, has_side_effects=True, vmem_limit_bytes=63 * 1024 * 1024),
        cost_estimate=pl.CostEstimate(flops=48 * rows * width * units, bytes_accessed=4 * rows * ctx * dim + 10 * width * width, transcendentals=0),
        name='layer',
    )(hidden_in, cache_len, freq, norm_attn, norm_mlp, k_cache, v_cache, w_q, w_k, w_v, w_o, w_gate, w_up, w_down)
    return hand_on(*results)


def hand_on_kernel(count, *refs):
    src, dst, buf, sem = refs[:count], refs[count:2 * count], refs[2 * count:3 * count], refs[3 * count]
    loads = [pltpu.make_async_copy(src[i], buf[i], sem.at[0, i]) for i in range(count)]
    stores = [pltpu.make_async_copy(buf[i], dst[i], sem.at[1, i]) for i in range(count)]
    for copy in loads:
        copy.start()
    for load, store in zip(loads, stores):
        load.wait()
        store.start()
    for copy in stores:
        copy.wait()


def hand_on(*arrays):
    hbm = pl.BlockSpec(memory_space=pl.ANY)
    return pl.pallas_call(
        functools.partial(hand_on_kernel, len(arrays)),
        out_shape=[jax.ShapeDtypeStruct(a.shape, a.dtype) for a in arrays],
        in_specs=[hbm] * len(arrays),
        out_specs=[hbm] * len(arrays),
        scratch_shapes=[pltpu.VMEM(a.shape, a.dtype) for a in arrays] + [pltpu.SemaphoreType.DMA((2, len(arrays)))],
        name='hand_on',
    )(*arrays)


def solution(mesh):
    row_spec = P(('dp', 'tp'), None)
    cache_spec = P(('dp', 'tp'), None, None)
    full_vec = P(None)
    full_mat = P(None, None)

    return jax.shard_map(
        layer,
        mesh=mesh,
        in_specs=(row_spec, cache_spec, cache_spec, P(('dp', 'tp')), full_vec, full_vec,
                  full_mat, full_mat, full_mat, full_mat, P(None, 'tp'), P(None, 'tp'), P('tp', None)),
        out_specs=(row_spec, row_spec, row_spec),
        check_vma=False,
    )
```

```python
import functools

import jax
import jax.numpy as jnp
import numpy as np
from jax import lax
from jax.experimental import pallas as pl
from jax.experimental.pallas import tpu as pltpu
from jax.sharding import PartitionSpec as P

MESH = pl.DeviceIdType.MESH


def layer_kernel(group, x_hbm, len_hbm, freq_hbm, gain_hbm, gain2_hbm, k_hbm, v_hbm, wq_hbm, wk_hbm, wv_hbm, wo_hbm,
                 wg_hbm, wu_hbm, wd_hbm, out_hbm, k_out, v_out,
                 x_ref, len_ref, freq_ref, gain_ref, gain2_ref, out_ref, k_ref, v_ref, wg, wu, wd, kbuf, vbuf, xs, qbuf, obuf, sbuf, knew, vnew, turn, x1, xb, hid, own, snd, prt, ring,
                 x_sem, y_sem, w_sem, q_sem, kv_sem, o_sem, k_sem, v_sem, ag_send, ag_recv, d_send, d_recv, r_send, r_recv):
    chips = lax.axis_size('tp') // 2
    me = lax.axis_index('tp')
    core = lax.rem(me, 2)
    chip = me // 2
    partner = me + 1 - 2 * core
    ahead = 2 * lax.rem(chip + 1, chips) + core
    behind = 2 * lax.rem(chip + chips - 1, chips) + core

    rows, width = x_ref.shape
    dim = wk_hbm.shape[1]
    heads = wq_hbm.shape[1] // dim
    ctx = k_hbm.shape[1]
    slots = kbuf.shape[0]
    groups = rows // group
    n_tile, _, tile = wg.shape
    side = rows // 2
    quart = rows // 4
    half = dim // 2
    per_part = groups // 2
    per_side = per_part // 2

    barrier = pltpu.get_barrier_semaphore()
    for dev in (partner, ahead, behind):
        pl.semaphore_signal(barrier, inc=1, device_id={'tp': dev}, device_id_type=MESH)

    def fetch(hbm, buf, n, sem):
        return pltpu.make_async_copy(hbm.at[:, pl.ds(pl.multiple_of(n * tile, tile), tile)], buf.at[n], sem)

    def q_load(n):
        return fetch(wq_hbm, wd, n, q_sem.at[n])

    def o_load(n):
        return fetch(wo_hbm, wu, n, o_sem.at[n])

    def gate_load(n):
        return fetch(wg_hbm, wg, n, w_sem.at[0, n])

    def up_load(n):
        return fetch(wu_hbm, wu, n, w_sem.at[1, n])

    def down_load(n):
        return fetch(wd_hbm, wd, n, w_sem.at[2, n])

    def kv_load(i):
        return pltpu.make_async_copy((wk_hbm, wv_hbm)[i], wg.at[0, :, pl.ds(i * dim, dim)], kv_sem.at[i])

    def first_row(g):
        j = lax.rem(g, per_part)
        return pl.multiple_of((j // per_side) * side + (g // per_part) * quart + lax.rem(j, per_side) * group, group)

    def k_load(g):
        slot = lax.rem(g, slots)
        return pltpu.make_async_copy(k_hbm.at[pl.ds(first_row(g), group)], kbuf.at[slot], k_sem.at[slot])

    def v_load(g):
        slot = lax.rem(g, slots)
        return pltpu.make_async_copy(v_hbm.at[pl.ds(first_row(g), group)], vbuf.at[slot], v_sem.at[slot])

    def to(src, dst, send, recv, dev):
        return pltpu.make_async_remote_copy(src_ref=src, dst_ref=dst, send_sem=send, recv_sem=recv,
                                            device_id={'tp': dev}, device_id_type=MESH)

    small = [pltpu.make_async_copy(src, dst, x_sem.at[i]) for i, (src, dst) in enumerate(
        ((x_hbm, x_ref), (gain_hbm, gain_ref), (len_hbm, len_ref), (freq_hbm, freq_ref), (gain2_hbm, gain2_ref)))]
    for copy in small:
        copy.start()
    kv_load(0).start()
    kv_load(1).start()
    for n in range(n_tile):
        q_load(n).start()
    for g in range(slots):
        k_load(g).start()
        v_load(g).start()

    for copy in small:
        copy.wait()
    xw = x_ref[...].astype(jnp.float32)
    inv = lax.rsqrt(jnp.mean(xw * xw, axis=-1, keepdims=True) + 1e-6)
    xs[...] = (xw * inv * (1.0 + gain_ref[...].astype(jnp.float32)[None])).astype(jnp.bfloat16)
    for r in range(rows):
        turn[pl.ds(r, 1), :] = len_ref[r].astype(jnp.float32) * freq_ref[...]
    angle = turn[...]
    cos_t, sin_t = jnp.cos(angle), jnp.sin(angle)

    def rotate(a, b):
        return a * cos_t - b * sin_t, b * cos_t + a * sin_t

    kv_load(0).wait()
    kk = jnp.dot(xs[...], wg[0, :, 0:dim], preferred_element_type=jnp.float32)
    ka, kb = rotate(kk[:, :half], kk[:, half:])
    ka, kb = ka.astype(jnp.bfloat16), kb.astype(jnp.bfloat16)
    k_ref[:, :half] = ka
    k_ref[:, half:] = kb
    knew[:, :half] = ka.astype(jnp.float32)
    knew[:, half:] = kb.astype(jnp.float32)
    kv_load(1).wait()
    vv = jnp.dot(xs[...], wg[0, :, dim:2 * dim], preferred_element_type=jnp.float32).astype(jnp.bfloat16)
    v_ref[...] = vv
    vnew[...] = vv.astype(jnp.float32)
    outs = [pltpu.make_async_copy(k_ref, k_out, y_sem.at[0]), pltpu.make_async_copy(v_ref, v_out, y_sem.at[1])]
    for copy in outs:
        copy.start()

    scale = dim ** -0.5
    for n in range(n_tile):
        q_load(n).wait()
        ql = jnp.dot(xs[...], wd[n], preferred_element_type=jnp.float32)
        for i in range(tile // dim):
            h = n * (tile // dim) + i
            qa, qb = rotate(ql[:, i * dim:i * dim + half], ql[:, i * dim + half:(i + 1) * dim])
            qbuf[0, pl.ds(h, rows, stride=heads), :] = (qa * scale).astype(jnp.bfloat16).astype(jnp.float32)
            qbuf[1, pl.ds(h, rows, stride=heads), :] = (qb * scale).astype(jnp.bfloat16).astype(jnp.float32)

    spots = lax.broadcasted_iota(jnp.int32, (heads, ctx), 1)

    def scores(g):
        slot = lax.rem(g, slots)
        base = first_row(lax.rem(g, groups))
        for i in range(group):
            spot = pl.ds(pl.multiple_of((base + i) * heads, heads), heads)
            q = jnp.concatenate([qbuf[0, spot, :], qbuf[1, spot, :]], axis=1).astype(jnp.bfloat16)
            sbuf[lax.rem(g, 2), i] = lax.dot_general(q, kbuf[slot, i], (((1,), (1,)), ((), ())), preferred_element_type=jnp.float32)

    def values(g):
        slot = lax.rem(g, slots)
        base = first_row(g)
        for i in range(group):
            r = base + i
            spot = pl.ds(pl.multiple_of(r * heads, heads), heads)
            k_row = knew[pl.ds(r, 1), :]
            v_row = vnew[pl.ds(r, 1), :]
            new = jnp.sum(qbuf[0, spot, :] * k_row[:, :half] + qbuf[1, spot, :] * k_row[:, half:], axis=1, keepdims=True)
            valid = spots < len_ref[r]
            s = jnp.where(valid, sbuf[lax.rem(g, 2), i], -jnp.inf)
            peak = jnp.maximum(jnp.max(s, axis=1, keepdims=True), new)
            w = jnp.exp(s - peak)
            new_w = jnp.exp(new - peak)
            total = jnp.sum(w, axis=1, keepdims=True) + new_w
            prob = (w / total).astype(jnp.bfloat16)
            new_p = (new_w / total).astype(jnp.bfloat16).astype(jnp.float32)
            o = jnp.dot(prob, vbuf[slot, i], preferred_element_type=jnp.float32) + new_p * v_row
            to_spot = pl.ds(pl.multiple_of((lax.rem(g, per_part) * group + i) * heads, heads), heads)
            obuf[0, to_spot, :] = o[:, :half]
            obuf[1, to_spot, :] = o[:, half:]

    def attend(g, carry):
        @pl.when(g + 1 < groups)
        def _():
            k_load(g + 1).wait()
        v_load(g).wait()
        scores(g + 1)
        values(g)
        @pl.when(g + slots < groups)
        def _():
            v_load(g + slots).start()
        @pl.when(g + 1 + slots < groups)
        def _():
            k_load(g + 1 + slots).start()
        @pl.when(g < n_tile)
        def _():
            o_load(g).start()
        @pl.when(g >= groups - n_tile)
        def _():
            gate_load(g - (groups - n_tile)).start()
        return carry

    def place(s, kind):
        return {'direct': ((0, 0), (2, 2)), 'end': ((0, 2), (3, 0)), 'far': ((1, 0), (2, 0)), 'own': ((1, 2), (3, 2))}[kind][s]

    def own_at(s):
        return place(s, 'own')

    def finish(s):
        for h in range(heads):
            spot = pl.ds(h, side, stride=heads)
            xs[0:side, h * dim:h * dim + half] = obuf[0, spot, :].astype(jnp.bfloat16)
            xs[0:side, h * dim + half:(h + 1) * dim] = obuf[1, spot, :].astype(jnp.bfloat16)
        a, b = pl.ds(s * quart, quart), pl.ds(side + s * quart, quart)

        def project(n, carry):
            if s == 0:
                o_load(n).wait()
            cols = pl.ds(pl.multiple_of(n * tile, tile), tile)
            mixed = jnp.dot(xs[0:side, :], wu[n], preferred_element_type=jnp.float32)
            x1[a, cols] = x_ref[a, cols].astype(jnp.float32) + mixed[0:quart]
            x1[b, cols] = x_ref[b, cols].astype(jnp.float32) + mixed[quart:side]
            if s == 1:
                up_load(n).start()
            return carry
        lax.fori_loop(0, n_tile, project, 0, unroll=True)
        if s == 1:
            arrive(0, 1, 3)
            gather(0, 7).start()
        for j, part in ((0, a), (1, b)):
            mid = x1[part, :]
            inv = lax.rsqrt(jnp.mean(mid * mid, axis=-1, keepdims=True) + 1e-6)
            normed = (mid * inv * (1.0 + gain2_ref[...].astype(jnp.float32)[None])).astype(jnp.bfloat16)
            spot = own_at(s)[1] + j
            xb[own_at(s)[0], spot * quart:(spot + 1) * quart, :] = normed

    def span(i, n=1):
        return pl.ds(i * quart, n * quart)

    def gather(s, i):
        def at(kind, k, n=1):
            b, first = place(s, kind)
            return xb.at[b, span(first + k, n)]

        def both(kind):
            b, first = place(s, kind)
            return at(kind, 0, 2), xb.at[b, span(first + 4, 2)], partner

        src, dst, dev = (
            (at('own', 0), at('direct', 1), ahead),
            (at('own', 1), at('end', 1), ahead),
            (at('own', 1), at('direct', 0), behind),
            (at('own', 0), at('end', 0), behind),
            (at('direct', 1), at('far', 0), ahead),
            (at('direct', 0), at('far', 1), behind),
            both('direct'),
            both('end'),
            both('far'),
            both('own'),
        )[i]
        return to(src, dst, ag_send.at[s, i], ag_recv.at[s, i], dev)

    def send(s):
        for i in (0, 2, 1, 3, 9):
            gather(s, i).start()

    def arrive(s, *ids):
        for i in ids:
            gather(s, i).wait_recv()

    def forward(s):
        arrive(s, 0, 2)
        for i in (4, 5, 6):
            gather(s, i).start()

    k_load(0).wait()
    scores(0)
    k_load(slots).start()
    lax.fori_loop(0, per_part, attend, 0)
    finish(0)
    pl.semaphore_wait(barrier, 3)
    send(0)
    lax.fori_loop(per_part, groups, attend, 0)
    forward(0)
    finish(1)
    for n in range(n_tile):
        down_load(n).start()
    send(1)

    def up_step(b, n):
        if b == 0:
            gate_load(n).wait()
            up_load(n).wait()
        gate = jnp.dot(xb[b], wg[n], preferred_element_type=jnp.float32)
        lin = jnp.dot(xb[b], wu[n], preferred_element_type=jnp.float32)
        hid[:, n * tile:(n + 1) * tile] = (jax.nn.gelu(gate, approximate=True) * lin).astype(jnp.bfloat16)

    def swap(b, n):
        return to(snd.at[b, n], prt.at[b, n], d_send.at[b, n], d_recv.at[b, n], partner)

    def hops(s, step, n):
        b, fwd = place(s, ('direct', 'far', 'end')[step])
        return (to(own.at[b, n, span(fwd)], ring.at[s, step, n, span(0)], r_send.at[s, step, 0, n], r_recv.at[s, step, 0, n], ahead),
                to(own.at[b, n, span(fwd + 1)], ring.at[s, step, n, span(1)], r_send.at[s, step, 1, n], r_recv.at[s, step, 1, n], behind))

    def merge(b, n):
        swap(b, n).wait_recv()
        own[b, n] = own[b, n] + prt[b, n]
        for s, step in (((0, 0),), ((0, 1),), ((1, 1), (1, 0)), ())[b]:
            for copy in hops(s, step, n):
                copy.start()

    pending = []

    def flush(keep=0, after=None):
        while len(pending) > keep:
            b, n = pending.pop(0)
            merge(b, n)
            if after is not None:
                after(n)

    def up(b, after=None):
        for n in range(n_tile):
            up_step(b, n)
            flush()
            if after is not None:
                after(n)

    def down(b, after=None):
        for n in range(n_tile):
            if b == 0:
                down_load(n).wait()
            part = jnp.dot(hid[...], wd[n], preferred_element_type=jnp.float32)
            own[b, n] = part[0:rows]
            snd[b, n] = part[rows:2 * rows]
            swap(b, n).start()
            pending.append((b, n))
            flush(2, after)

    def relay(s, n):
        for copy in hops(s, 1, n):
            copy.wait_recv()
        b, first = place(s, 'end')
        own[b, n, span(first, 2)] = own[b, n, span(first, 2)] + ring[s, 1, n]
        for copy in hops(s, 2, n):
            copy.start()

    def settle(s, n):
        for step in (0, 2):
            for copy in hops(s, step, n):
                copy.wait_recv()
        cols = slice(n * tile, (n + 1) * tile)
        a, b = pl.ds(s * quart, quart), pl.ds(side + s * quart, quart)
        mine, first = place(s, 'own')
        out_ref[a, cols] = (x1[a, cols] + (own[mine, n, span(first)] + (ring[s, 0, n, span(1)] + ring[s, 2, n, span(0)]))).astype(jnp.bfloat16)
        out_ref[b, cols] = (x1[b, cols] + (own[mine, n, span(first + 1)] + (ring[s, 0, n, span(0)] + ring[s, 2, n, span(1)]))).astype(jnp.bfloat16)

    def give(s):
        a, b = pl.ds(s * quart, quart), pl.ds(side + s * quart, quart)
        for j, part in enumerate((a, b)):
            copy = pltpu.make_async_copy(out_ref.at[part], out_hbm.at[part], y_sem.at[2 + 2 * s + j])
            copy.start()
            outs.append(copy)

    arrive(0, 6, 7)
    up(0)
    forward(1)
    arrive(0, 4, 5)
    gather(0, 8).start()
    down(0)
    arrive(1, 1, 3)
    gather(1, 7).start()
    arrive(0, 8, 9)
    up(1)
    arrive(1, 4, 5)
    gather(1, 8).start()
    down(1)
    arrive(1, 6, 8)
    up(2, lambda n: relay(0, n))
    down(2)
    arrive(1, 7, 9)
    up(3)
    down(3, lambda n: relay(1, n))
    for n in range(n_tile):
        settle(0, n)
    give(0)
    flush(0, lambda n: relay(1, n))
    for n in range(n_tile):
        settle(1, n)
    give(1)

    for s in range(2):
        for i in range(10):
            gather(s, i).wait_send()

    def drain(n, carry):
        for b in range(4):
            swap(b, n).wait_send()
        for s in range(2):
            for step in range(3):
                for copy in hops(s, step, n):
                    copy.wait_send()
        return carry
    lax.fori_loop(0, n_tile, drain, 0)
    for copy in outs:
        copy.wait()


def layer(hidden_in, k_cache, v_cache, cache_len, norm_attn, norm_mlp, w_q, w_k, w_v, w_o, w_gate, w_up, w_down):
    rows, width = hidden_in.shape
    ctx, dim = k_cache.shape[1:]
    heads = w_q.shape[1] // dim
    units = w_gate.shape[1]
    group, slots, tile = 8, 4, 512
    n_tile = width // tile
    assert heads * dim == width and units == width
    sems = pltpu.SemaphoreType.DMA
    bf16, f32 = jnp.bfloat16, jnp.float32
    hbm = pl.BlockSpec(memory_space=pl.ANY)
    freq = np.float32(10000.0 ** (-2.0 * np.arange(dim // 2) / dim))[None]
    results = pl.pallas_call(
        functools.partial(layer_kernel, group),
        out_shape=[jax.ShapeDtypeStruct((rows, width), bf16)] + [jax.ShapeDtypeStruct((rows, dim), bf16)] * 2,
        in_specs=[hbm] * 14,
        out_specs=[hbm] * 3,
        scratch_shapes=[
            pltpu.VMEM((rows, width), bf16),
            pltpu.SMEM((rows,), jnp.int32),
            pltpu.VMEM((1, dim // 2), f32),
            pltpu.VMEM((width,), bf16),
            pltpu.VMEM((width,), bf16),
            pltpu.VMEM((rows, width), bf16),
            pltpu.VMEM((rows, dim), bf16),
            pltpu.VMEM((rows, dim), bf16),
            pltpu.VMEM((n_tile, width, tile), bf16),
            pltpu.VMEM((n_tile, width, tile), bf16),
            pltpu.VMEM((n_tile, units, tile), bf16),
            pltpu.VMEM((slots, group, ctx, dim), bf16),
            pltpu.VMEM((slots, group, ctx, dim), bf16),
            pltpu.VMEM((rows, width), bf16),
            pltpu.VMEM((2, rows * heads, dim // 2), f32),
            pltpu.VMEM((2, rows * heads // 2, dim // 2), f32),
            pltpu.VMEM((2, group, heads, ctx), f32),
            pltpu.VMEM((rows, dim), f32),
            pltpu.VMEM((rows, dim), f32),
            pltpu.VMEM((rows, dim // 2), f32),
            pltpu.VMEM((rows, width), f32),
            pltpu.VMEM((4, 2 * rows, width), bf16),
            pltpu.VMEM((2 * rows, units), bf16),
            pltpu.VMEM((4, n_tile, rows, tile), f32),
            pltpu.VMEM((4, n_tile, rows, tile), f32),
            pltpu.VMEM((4, n_tile, rows, tile), f32),
            pltpu.VMEM((2, 3, n_tile, rows // 2, tile), f32),
            sems((5,)), sems((6,)), sems((3, n_tile)), sems((n_tile,)), sems((2,)), sems((n_tile,)), sems((slots,)), sems((slots,)),
            sems((2, 10)), sems((2, 10)),
            sems((4, n_tile)), sems((4, n_tile)),
            sems((2, 3, 2, n_tile)), sems((2, 3, 2, n_tile)),
        ],
        compiler_params=pltpu.CompilerParams(collective_id=0, has_side_effects=True, vmem_limit_bytes=63 * 1024 * 1024),
        cost_estimate=pl.CostEstimate(flops=48 * rows * width * units, bytes_accessed=4 * rows * ctx * dim + 10 * width * width, transcendentals=0),
        name='layer',
    )(hidden_in, cache_len, freq, norm_attn, norm_mlp, k_cache, v_cache, w_q, w_k, w_v, w_o, w_gate, w_up, w_down)
    return hand_on(*results)


def hand_on_kernel(count, *refs):
    src, dst, buf, sem = refs[:count], refs[count:2 * count], refs[2 * count:3 * count], refs[3 * count]
    loads = [pltpu.make_async_copy(src[i], buf[i], sem.at[0, i]) for i in range(count)]
    stores = [pltpu.make_async_copy(buf[i], dst[i], sem.at[1, i]) for i in range(count)]
    for copy in loads:
        copy.start()
    for load, store in zip(loads, stores):
        load.wait()
        store.start()
    for copy in stores:
        copy.wait()


def hand_on(*arrays):
    hbm = pl.BlockSpec(memory_space=pl.ANY)
    return pl.pallas_call(
        functools.partial(hand_on_kernel, len(arrays)),
        out_shape=[jax.ShapeDtypeStruct(a.shape, a.dtype) for a in arrays],
        in_specs=[hbm] * len(arrays),
        out_specs=[hbm] * len(arrays),
        scratch_shapes=[pltpu.VMEM(a.shape, a.dtype) for a in arrays] + [pltpu.SemaphoreType.DMA((2, len(arrays)))],
        name='hand_on',
    )(*arrays)


def solution(mesh):
    row_spec = P(('dp', 'tp'), None)
    cache_spec = P(('dp', 'tp'), None, None)
    full_vec = P(None)
    full_mat = P(None, None)

    return jax.shard_map(
        layer,
        mesh=mesh,
        in_specs=(row_spec, cache_spec, cache_spec, P(('dp', 'tp')), full_vec, full_vec,
                  full_mat, full_mat, full_mat, full_mat, P(None, 'tp'), P(None, 'tp'), P('tp', None)),
        out_specs=(row_spec, row_spec, row_spec),
        check_vma=False,
    )
```
